32 devices in a mesh: brick: 16 (over z, y, core), chan: 2 (over x).
Axes of the slice: x: 2, y: 2, z: 4, core: 2. Of those that a mesh axis runs over, the one named last changes fastest.
Arguments:
- volume: bfloat16 [32, 16, 64, 256], P('brick', 'chan'), may hold values from -6 to 6
- first_weight: bfloat16 [3, 3, 3, 256, 256], replicated, may hold values from -0.078125 to 0.078125
- second_weight: bfloat16 [3, 3, 3, 256, 256], replicated, may hold values from -0.078125 to 0.078125
- coarse_weight: bfloat16 [3, 3, 3, 256, 512], P(None, None, None, None, 'chan'), may hold values from -0.078125 to 0.078125
- projection: bfloat16 [512, 256], P('chan'), may hold values from -0.25 to 0.25
Outputs:
- merged: bfloat16 [32, 16, 64, 256], P('brick', 'chan')
The draws below stay inside these ranges and needn't reach their ends.
All inputs are finite; a program needn't handle non-finite values.
Results may differ from the reference program's by a relative error of at most 0.011.
Values may be sent and summed in bfloat16 or wider, within the bound.
No kernel may reach another device: no remote copies, remote signals or barrier semaphores. Data moves between devices by JAX's collectives and lax.ppermute only.
A program may use at most 64 MiB of HBM per device.

```python
import jax
import jax.numpy as jnp
from jax import lax

C = 256
CO = 512
NZ = 64
NX = 32
NY = 16


def steps_of(stream_key, shape, split, least, high):
    gain = 1.0
    for dim, parts in split:
        draws = jax.random.uniform(jax.random.fold_in(jax.random.fold_in(stream_key, 6), dim), (parts,), jnp.float32, least / len(split), high / len(split))
        gain = gain * jnp.repeat(jnp.exp(draws), shape[dim] // parts).reshape((-1,) + (1,) * (len(shape) - 1 - dim))
    return gain


def noise(own_key, extent, deviation, bound, split=(), dtype=jnp.bfloat16):
    values = jax.random.normal(own_key, extent, jnp.float32) * deviation
    if len(split) > 0:
        values = steps_of(own_key, extent, split, -0.22, 0.18) * values
    return jnp.clip(values, min=-bound, max=bound).astype(dtype)


def setup_inputs(seed: int = 0) -> dict:
    key_of = jax.random.split(jax.random.key(seed), 6)
    volume = noise(key_of[0], (NX, NY, NZ, C), 1.0, 6.0, ((0, 16), (1, 2)))
    first_weight = noise(key_of[1], (3, 3, 3, C, C), (27 * C) ** -0.5, 0.078125)
    second_weight = noise(key_of[2], (3, 3, 3, C, C), (27 * C) ** -0.5, 0.078125)
    coarse_weight = noise(key_of[3], (3, 3, 3, C, CO), (27 * C) ** -0.5, 0.078125, ((4, 2),))
    projection = noise(key_of[4], (CO, C), CO ** -0.5, 0.25, ((0, 2),))
    return {"volume": volume, "first_weight": first_weight, "second_weight": second_weight, "coarse_weight": coarse_weight, "projection": projection}


def convolve(field, weight):
    source = field.astype(jnp.float32)[None]
    kernel = weight.astype(jnp.float32)
    result = lax.conv_general_dilated(source, kernel, (1, 1, 1), "SAME", dimension_numbers=("NDHWC", "DHWIO", "NDHWC"), precision=lax.Precision.HIGHEST)
    return result[0]


def reference(volume, first_weight, second_weight, coarse_weight, projection):
    layer_one = jnp.maximum(convolve(volume, first_weight), 0.0).astype(jnp.bfloat16)
    skipped = jnp.maximum(convolve(layer_one, second_weight), 0.0).astype(jnp.bfloat16)
    size_x, size_y, size_z, channels_in = skipped.shape
    blocks = skipped.astype(jnp.float32).reshape(size_x // 2, 2, size_y // 2, 2, size_z // 2, 2, channels_in)
    pooled = jnp.mean(blocks, axis=(1, 3, 5)).astype(jnp.bfloat16)
    coarse = jnp.maximum(convolve(pooled, coarse_weight), 0.0).astype(jnp.bfloat16)
    flat = coarse.reshape(-1, coarse.shape[3])
    lifted = jnp.dot(flat, projection, preferred_element_type=jnp.float32).reshape(size_x // 2, size_y // 2, size_z // 2, channels_in)
    upsampled = jnp.repeat(jnp.repeat(jnp.repeat(lifted, 2, axis=0), 2, axis=1), 2, axis=2)
    return (skipped.astype(jnp.float32) + upsampled).astype(jnp.bfloat16)
```

```python
import functools

import jax
import jax.numpy as jnp
from jax import lax
from jax.experimental import pallas as pl
from jax.experimental.pallas import tpu as pltpu
from jax.sharding import PartitionSpec as P


AXES = ("brick", "chan")
BF16 = jnp.bfloat16
F32 = jnp.float32
LANES = 128
VMEM_SPEC = pl.BlockSpec(memory_space=pltpu.VMEM)


def brick_partner(kind, brick, bricks):
    if kind == "own":
        return brick
    partner = brick ^ 1 if kind == "near" else ((brick + 1) ^ 1) - 1
    return partner if 0 <= partner < bricks else None


def exchange(value, kind, chan_of):
    bricks, chans = lax.axis_size("brick"), lax.axis_size("chan")
    pairs = []
    for brick in range(bricks):
        for chan in range(chans):
            other, target = brick_partner(kind, brick, bricks), chan_of(chan)
            if other is not None and target is not None and 0 <= target < chans:
                pairs.append((brick * chans + chan, other * chans + target))
    return lax.ppermute(value, AXES, pairs)


def call(kernel, inputs, outputs, scratch, name, flops, limit_mib, results_in_vmem=True):
    inputs = [pltpu.with_memory_space_constraint(value, pltpu.VMEM) for value in inputs]
    if results_in_vmem:
        out_shape = [pltpu.VMEM(shape, dtype) for shape, dtype in outputs]
    else:
        out_shape = [jax.ShapeDtypeStruct(shape, dtype) for shape, dtype in outputs]
    return pl.pallas_call(
        kernel,
        out_shape=out_shape,
        in_specs=[VMEM_SPEC] * len(inputs),
        out_specs=[VMEM_SPEC] * len(outputs),
        scratch_shapes=scratch,
        name=name,
        compiler_params=pltpu.CompilerParams(vmem_limit_bytes=limit_mib * 2**20),
        cost_estimate=pl.CostEstimate(flops=flops, bytes_accessed=2**20, transcendentals=0),
    )(*inputs)


def tile_of(rows):
    return max(lines for lines in range(1, 10) if rows % lines == 0)


def conv_lines(terms, row, lines, weight):
    sums = []
    for dz in range(3):
        total = None
        for ref, plane, dx in terms:
            for dy in range(3):
                window = ref[plane, pl.ds(row + dy, lines)]
                window = window.reshape(lines * window.shape[1], window.shape[2])
                part = jnp.dot(window, weight[dx, dy, dz], preferred_element_type=F32)
                total = part if total is None else total + part
        sums.append(total)
    depth = terms[0][0].shape[2]
    count = sums[0].shape[0]
    place = lax.rem(lax.broadcasted_iota(jnp.int32, sums[0].shape, 0), depth)
    before = jnp.where(place == 0, 0.0, pltpu.roll(sums[0], 1, 0))
    after = jnp.where(place == depth - 1, 0.0, pltpu.roll(sums[2], count - 1, 0))
    return (before + sums[1] + after).reshape(lines, depth, sums[0].shape[1])


def tap(step, odd):
    return step + odd * (2 - 2 * step)


def halo_plan(chans, size_y):
    chan = lax.axis_index("chan")
    if chans == 1:
        return []
    if chans == 2:
        return [(jnp.where(chan == 1, 0, size_y + 2), jnp.where(chan == 1, size_y + 2, 0))]
    return [(0, None), (size_y + 2, None)]


def fill_planes(target, slot, plane, block, halos, chans):
    size_y = block.shape[1]
    target[slot, 2 : size_y + 2] = block[plane]
    zeros = jnp.zeros((2,) + target.shape[2:], target.dtype)
    if chans == 1:
        target[slot, 0:2] = zeros
        target[slot, size_y + 2 : size_y + 4] = zeros
    for (place, empty), halo in zip(halo_plan(chans, size_y), halos):
        target[slot, pl.ds(place, 2)] = halo[plane]
        if empty is not None:
            target[slot, pl.ds(empty, 2)] = zeros


def first_row(chans):
    if chans == 1:
        return 0
    if chans == 2:
        return -lax.axis_index("chan")
    return -1


def clear_outside(layer, slot, chans):
    chan = lax.axis_index("chan")
    last = layer.shape[1] - 1
    for row, owner in ((0, 0), (last, chans - 1)):
        if chans <= 2:
            keep = jnp.logical_and(chans == 2, chan != owner)
        else:
            keep = chan != owner
        layer[slot, row] = jnp.where(keep, layer[slot, row], jnp.zeros_like(layer[slot, row]))


def kernel_a(*refs, chans, halo_count):
    own, own_halos = refs[0], refs[1 : 1 + halo_count]
    near, near_halos = refs[1 + halo_count], refs[2 + halo_count : 2 + 2 * halo_count]
    weight_one, weight_two, layer_far, layer_own, out_far, out_near, field, layer = refs[2 + 2 * halo_count :]
    odd = lax.rem(lax.axis_index("brick"), 2)
    size_y = own.shape[1]
    fill_planes(field, 0, odd, own, own_halos, chans)
    fill_planes(field, 1, 1 - odd, own, own_halos, chans)
    fill_planes(field, 2, odd, near, near_halos, chans)
    fill_planes(field, 3, 1 - odd, near, near_halos, chans)
    start = first_row(chans)
    rows = layer_far.shape[0]
    lines = tile_of(rows)
    for row in range(0, rows, lines):
        base = start + row + 1
        for slot in range(2):
            terms = [(field, slot + step, tap(step, odd)) for step in range(3)]
            value = jnp.maximum(conv_lines(terms, base, lines, weight_one), 0.0).astype(BF16)
            layer[slot, pl.ds(start + row + 1, lines)] = value
    for slot in range(2):
        clear_outside(layer, slot, chans)
    lines_out = tile_of(size_y)
    for row in range(0, size_y, lines_out):
        out_far[pl.ds(row, lines_out)] = conv_lines([(layer, 0, tap(2, odd))], row, lines_out, weight_two)
        out_near[pl.ds(row, lines_out)] = conv_lines(
            [(layer, 0, tap(1, odd)), (layer, 1, tap(2, odd))], row, lines_out, weight_two
        )
    for row in range(0, rows, lines):
        base = start + row + 1
        layer_own[pl.ds(row, lines)] = conv_lines(
            [(field, 0, tap(1, odd)), (field, 1, tap(2, odd))], base, lines, weight_one
        )
        layer_far[pl.ds(row, lines)] = conv_lines([(field, 0, tap(2, odd))], base, lines, weight_one)


def kernel_b(*refs, chans, halo_count):
    far, far_halos = refs[0], refs[1 : 1 + halo_count]
    layer_far, layer_own, out_far, out_near, weight_one, weight_two = refs[1 + halo_count : 7 + halo_count]
    skipped, pooled, field, layer, sums = refs[7 + halo_count :]
    brick = lax.axis_index("brick")
    odd = lax.rem(brick, 2)
    size_y, depth = far.shape[1], far.shape[2]
    fill_planes(field, 0, odd, far, far_halos, chans)
    fill_planes(field, 1, 1 - odd, far, far_halos, chans)
    inside = jnp.logical_and(brick + odd > 0, brick + odd < lax.axis_size("brick"))
    start = first_row(chans)
    rows = layer_far.shape[0]
    lines = tile_of(rows)
    for row in range(0, rows, lines):
        base = start + row + 1
        value = conv_lines([(field, 0, tap(0, odd)), (field, 1, tap(1, odd))], base, lines, weight_one)
        value = jnp.maximum(value + layer_far[pl.ds(row, lines)], 0.0)
        layer[0, pl.ds(base, lines)] = jnp.where(inside, value, 0.0).astype(BF16)
        value = conv_lines([(field, 1, tap(0, odd))], base, lines, weight_one)
        value = jnp.maximum(value + layer_own[pl.ds(row, lines)], 0.0)
        layer[1, pl.ds(base, lines)] = value.astype(BF16)
    for slot in range(2):
        clear_outside(layer, slot, chans)
    lines_out = tile_of(size_y)
    for row in range(0, size_y, lines_out):
        spot = pl.ds(row, lines_out)
        value = conv_lines([(layer, 0, tap(0, odd)), (layer, 1, tap(1, odd))], row, lines_out, weight_two)
        first = jnp.maximum(value + out_far[spot], 0.0).astype(BF16)
        skipped[odd, spot] = first
        value = conv_lines([(layer, 1, tap(0, odd))], row, lines_out, weight_two)
        second = jnp.maximum(value + out_near[spot], 0.0).astype(BF16)
        skipped[1 - odd, spot] = second
        both = first.astype(F32) + second.astype(F32)
        for group in range(sums.shape[0]):
            sums[group, spot] = both[:, :, group * LANES : (group + 1) * LANES]
    for row in range(size_y // 2):
        for group in range(sums.shape[0]):
            pairs = [
                sums[group, 2 * row + step, pl.ds(side, depth // 2, stride=2)] for step in range(2) for side in range(2)
            ]
            mean = (pairs[0] + pairs[1] + pairs[2] + pairs[3]) * 0.125
            pooled[row, :, group * LANES : (group + 1) * LANES] = mean.astype(BF16)


def kernel_c(*refs, chans):
    blocks = refs[: 3 * chans]
    weight, projection = refs[3 * chans : 3 * chans + 2]
    own_part, sent = refs[3 * chans + 2], refs[3 * chans + 3 : 4 * chans + 2]
    field, parts = refs[4 * chans + 2 :]
    odd = lax.rem(lax.axis_index("brick"), 2)
    chan = lax.axis_index("chan")
    rows, depth = blocks[0].shape[0], blocks[0].shape[1]
    total = chans * rows
    for plane in range(3):
        zeros = jnp.zeros(field.shape[2:], field.dtype)
        field[plane, 0] = zeros
        field[plane, total + 1] = zeros
        for step in range(chans):
            source = lax.rem(chan - step + chans, chans)
            field[plane, pl.ds(1 + source * rows, rows)] = blocks[plane * chans + step][...]
    lines = tile_of(total)
    for row in range(0, total, lines):
        value = conv_lines([(field, step, tap(step, odd)) for step in range(3)], row, lines, weight)
        value = jnp.maximum(value, 0.0).astype(BF16).reshape(lines * depth, weight.shape[4])
        part = jnp.dot(value, projection[...], preferred_element_type=F32)
        parts[pl.ds(row, lines)] = part.reshape(lines, depth, part.shape[1])
    own_part[...] = parts[pl.ds(chan * rows, rows)]
    for step in range(1, chans):
        target = lax.rem(chan + step, chans)
        sent[step - 1][...] = parts[pl.ds(target * rows, rows)].astype(BF16)


def kernel_d(*refs):
    skipped, own_part = refs[0], refs[1]
    received, merged, fine = refs[2:-2], refs[-2], refs[-1]
    rows, depth = own_part.shape[0], own_part.shape[1]
    lifted = own_part[...]
    for part in received:
        lifted = lifted + part[...].astype(F32)
    for group in range(fine.shape[0]):
        lanes = slice(group * LANES, (group + 1) * LANES)
        for row in range(rows):
            for side in range(2):
                fine[group, row, pl.ds(side, depth, stride=2)] = lifted[row, :, lanes]
        for row in range(rows):
            value = fine[group, row]
            for plane in range(2):
                for step in range(2):
                    line = 2 * row + step
                    merged[plane, line, :, lanes] = (skipped[plane, line, :, lanes].astype(F32) + value).astype(BF16)


def shards(volume, first_weight, second_weight, coarse_weight, projection):
    chans = lax.axis_size("chan")
    chan = lax.axis_index("chan")
    size_x, size_y, depth, channels = volume.shape
    assert size_x == 2 and lax.axis_size("brick") % 2 == 0

    if chans == 1:
        sides = []
    elif chans == 2:
        edge = lax.dynamic_slice_in_dim(volume, jnp.where(chan == 0, size_y - 2, 0), 2, axis=1)
        sides = [(edge, lambda c: 1 - c)]
    else:
        sides = [
            (lax.slice_in_dim(volume, size_y - 2, size_y, axis=1), lambda c: c + 1),
            (lax.slice_in_dim(volume, 0, 2, axis=1), lambda c: c - 1),
        ]
    far = exchange(volume, "far", lambda c: c)
    far_halos = [exchange(edge, "far", chan_of) for edge, chan_of in sides]
    own_halos = [exchange(edge, "own", chan_of) for edge, chan_of in sides]
    near_halos = [exchange(edge, "near", chan_of) for edge, chan_of in sides]
    near = exchange(volume, "near", lambda c: c)

    rows = size_y + min(chans - 1, 2)
    flops_of_plane = 2 * size_y * depth * 9 * channels * channels
    static = dict(chans=chans, halo_count=len(sides))
    partials = call(
        functools.partial(kernel_a, **static),
        [volume, *own_halos, near, *near_halos, first_weight, second_weight],
        [((rows, depth, channels), F32)] * 2 + [((size_y, depth, channels), F32)] * 2,
        [pltpu.VMEM((4, size_y + 4, depth, channels), BF16), pltpu.VMEM((2, size_y + 2, depth, channels), BF16)],
        "kernel_a",
        12 * flops_of_plane,
        16,
    )
    skipped, pooled = call(
        functools.partial(kernel_b, **static),
        [far, *far_halos, *partials, first_weight, second_weight],
        [(volume.shape, BF16), ((size_y // 2, depth // 2, channels), BF16)],
        [
            pltpu.VMEM((2, size_y + 4, depth, channels), BF16),
            pltpu.VMEM((2, size_y + 2, depth, channels), BF16),
            pltpu.VMEM((channels // LANES, size_y, depth, LANES), F32),
        ],
        "kernel_b",
        6 * flops_of_plane,
        16,
    )

    turns = [(lambda c, step=step: (c + step) % chans) for step in range(chans)]
    far_blocks = [exchange(pooled, "far", turn) for turn in turns]
    own_blocks = [pooled] + [exchange(pooled, "own", turn) for turn in turns[1:]]
    near_blocks = [exchange(pooled, "near", turn) for turn in turns]
    part_shape = (size_y // 2, depth // 2, channels)
    coarse_rows = chans * size_y // 2
    parts = call(
        functools.partial(kernel_c, chans=chans),
        [*far_blocks, *own_blocks, *near_blocks, coarse_weight, projection],
        [(part_shape, F32)] + [(part_shape, BF16)] * (chans - 1),
        [
            pltpu.VMEM((3, coarse_rows + 2, depth // 2, channels), BF16),
            pltpu.VMEM((coarse_rows, depth // 2, channels), F32),
        ],
        "kernel_c",
        2 * coarse_rows * (depth // 2) * 27 * channels * coarse_weight.shape[4],
        16,
    )
    received = [exchange(part, "own", turn) for part, turn in zip(parts[1:], turns[1:])]
    return call(
        kernel_d,
        [skipped, parts[0], *received],
        [(volume.shape, BF16)],
        [pltpu.VMEM((channels // LANES, size_y // 2, depth, LANES), F32)],
        "kernel_d",
        volume.size,
        16,
        results_in_vmem=False,
    )[0]


def solution(mesh):
    in_specs = (
        P("brick", "chan", None, None),
        P(),
        P(),
        P(None, None, None, None, "chan"),
        P("chan", None),
    )
    out_specs = P("brick", "chan", None, None)
    return jax.shard_map(shards, mesh=mesh, in_specs=in_specs, out_specs=out_specs, check_vma=False)
```

```python
import functools

import jax
import jax.numpy as jnp
from jax import lax
from jax.experimental import pallas as pl
from jax.experimental.pallas import tpu as pltpu
from jax.sharding import PartitionSpec as P


AXES = ("brick", "chan")
BF16 = jnp.bfloat16
F32 = jnp.float32
LANES = 128
WEIGHT_COPY_FLOPS = 2**33
VMEM_SPEC = pl.BlockSpec(memory_space=pltpu.VMEM)


def brick_partner(kind, brick, bricks):
    if kind == "own":
        return brick
    partner = brick ^ 1 if kind == "near" else ((brick + 1) ^ 1) - 1
    return partner if 0 <= partner < bricks else None


def exchange(value, kind, chan_of):
    bricks, chans = lax.axis_size("brick"), lax.axis_size("chan")
    pairs = []
    for brick in range(bricks):
        for chan in range(chans):
            other, target = brick_partner(kind, brick, bricks), chan_of(chan)
            if other is not None and target is not None and 0 <= target < chans:
                pairs.append((brick * chans + chan, other * chans + target))
    return lax.ppermute(value, AXES, pairs)


def send_edges(volume_ref, *edges, chans):
    chan = lax.axis_index("chan")
    size_y = volume_ref.shape[1]
    for index, edge in enumerate(edges):
        start = jnp.where(chan == 0, size_y - 2, 0) if chans == 2 else (size_y - 2) * (1 - index)
        edge[...] = volume_ref[:, pl.ds(start, 2)]


def call(kernel, inputs, outputs, scratch, flops, limit_mib, results_in_vmem=True):
    inputs = [pltpu.with_memory_space_constraint(value, pltpu.VMEM) for value in inputs]
    if results_in_vmem:
        out_shape = [pltpu.VMEM(shape, dtype) for shape, dtype in outputs]
    else:
        out_shape = [jax.ShapeDtypeStruct(shape, dtype) for shape, dtype in outputs]
    return pl.pallas_call(
        kernel,
        out_shape=out_shape,
        in_specs=[VMEM_SPEC] * len(inputs),
        out_specs=[VMEM_SPEC] * len(outputs),
        scratch_shapes=scratch,
        compiler_params=pltpu.CompilerParams(vmem_limit_bytes=limit_mib * 2**20),
        cost_estimate=pl.CostEstimate(flops=flops, bytes_accessed=2**20, transcendentals=0),
    )(*inputs)


def tile_of(rows):
    return max(lines for lines in range(1, 10) if rows % lines == 0)


def conv_lines(terms, row, lines, weight):
    sums = []
    for dz in range(3):
        total = None
        for ref, plane, dx in terms:
            for dy in range(3):
                window = ref[plane, pl.ds(row + dy, lines)]
                window = window.reshape(lines * window.shape[1], window.shape[2])
                part = jnp.dot(window, weight[dx, dy, dz], preferred_element_type=F32)
                total = part if total is None else total + part
        sums.append(total)
    depth = terms[0][0].shape[2]
    count = sums[0].shape[0]
    place = lax.rem(lax.broadcasted_iota(jnp.int32, sums[0].shape, 0), depth)
    before = jnp.where(place == 0, 0.0, pltpu.roll(sums[0], 1, 0))
    after = jnp.where(place == depth - 1, 0.0, pltpu.roll(sums[2], count - 1, 0))
    return (before + sums[1] + after).reshape(lines, depth, sums[0].shape[1])


def tap(step, odd):
    return step + odd * (2 - 2 * step)


def halo_plan(chans, size_y):
    chan = lax.axis_index("chan")
    if chans == 1:
        return []
    if chans == 2:
        return [(jnp.where(chan == 1, 0, size_y + 2), jnp.where(chan == 1, size_y + 2, 0))]
    return [(0, None), (size_y + 2, None)]


def fill_planes(target, slot, plane, block, halos, chans):
    size_y = block.shape[1]
    target[slot, 2 : size_y + 2] = block[plane]
    zeros = jnp.zeros((2,) + target.shape[2:], target.dtype)
    if chans == 1:
        target[slot, 0:2] = zeros
        target[slot, size_y + 2 : size_y + 4] = zeros
    for (place, empty), halo in zip(halo_plan(chans, size_y), halos):
        target[slot, pl.ds(place, 2)] = halo[plane]
        if empty is not None:
            target[slot, pl.ds(empty, 2)] = zeros


def first_row(chans):
    if chans == 1:
        return 0
    if chans == 2:
        return -lax.axis_index("chan")
    return -1


def clear_outside(layer, slot, chans):
    chan = lax.axis_index("chan")
    last = layer.shape[1] - 1
    for row, owner in ((0, 0), (last, chans - 1)):
        if chans <= 2:
            keep = jnp.logical_and(chans == 2, chan != owner)
        else:
            keep = chan != owner
        layer[slot, row] = jnp.where(keep, layer[slot, row], jnp.zeros_like(layer[slot, row]))


def kernel_a(*refs, chans, halo_count):
    own, own_halos = refs[0], refs[1 : 1 + halo_count]
    near, near_halos = refs[1 + halo_count], refs[2 + halo_count : 2 + 2 * halo_count]
    weight_one, weight_two, layer_far, layer_own, out_far, out_near, field, layer = refs[2 + 2 * halo_count :]
    odd = lax.rem(lax.axis_index("brick"), 2)
    size_y = own.shape[1]
    fill_planes(field, 0, odd, own, own_halos, chans)
    fill_planes(field, 1, 1 - odd, own, own_halos, chans)
    fill_planes(field, 2, odd, near, near_halos, chans)
    fill_planes(field, 3, 1 - odd, near, near_halos, chans)
    start = first_row(chans)
    rows = layer_far.shape[0]
    lines = tile_of(rows)
    for row in range(0, rows, lines):
        base = start + row + 1
        for slot in range(2):
            terms = [(field, slot + step, tap(step, odd)) for step in range(3)]
            value = jnp.maximum(conv_lines(terms, base, lines, weight_one), 0.0).astype(BF16)
            layer[slot, pl.ds(start + row + 1, lines)] = value
    for slot in range(2):
        clear_outside(layer, slot, chans)
    lines_out = tile_of(size_y)
    for row in range(0, size_y, lines_out):
        out_far[pl.ds(row, lines_out)] = conv_lines([(layer, 0, tap(2, odd))], row, lines_out, weight_two)
        out_near[pl.ds(row, lines_out)] = conv_lines(
            [(layer, 0, tap(1, odd)), (layer, 1, tap(2, odd))], row, lines_out, weight_two
        )
    for row in range(0, rows, lines):
        base = start + row + 1
        layer_own[pl.ds(row, lines)] = conv_lines(
            [(field, 0, tap(1, odd)), (field, 1, tap(2, odd))], base, lines, weight_one
        )
        layer_far[pl.ds(row, lines)] = conv_lines([(field, 0, tap(2, odd))], base, lines, weight_one)


def kernel_b(*refs, chans, halo_count):
    far, far_halos = refs[0], refs[1 : 1 + halo_count]
    layer_far, layer_own, out_far, out_near, weight_one, weight_two = refs[1 + halo_count : 7 + halo_count]
    skipped, pooled, field, layer, sums = refs[7 + halo_count :]
    brick = lax.axis_index("brick")
    odd = lax.rem(brick, 2)
    size_y, depth = far.shape[1], far.shape[2]
    fill_planes(field, 0, odd, far, far_halos, chans)
    fill_planes(field, 1, 1 - odd, far, far_halos, chans)
    inside = jnp.logical_and(brick + odd > 0, brick + odd < lax.axis_size("brick"))
    start = first_row(chans)
    rows = layer_far.shape[0]
    lines = tile_of(rows)
    for row in range(0, rows, lines):
        base = start + row + 1
        value = conv_lines([(field, 0, tap(0, odd)), (field, 1, tap(1, odd))], base, lines, weight_one)
        value = jnp.maximum(value + layer_far[pl.ds(row, lines)], 0.0)
        layer[0, pl.ds(base, lines)] = jnp.where(inside, value, 0.0).astype(BF16)
        value = conv_lines([(field, 1, tap(0, odd))], base, lines, weight_one)
        value = jnp.maximum(value + layer_own[pl.ds(row, lines)], 0.0)
        layer[1, pl.ds(base, lines)] = value.astype(BF16)
    for slot in range(2):
        clear_outside(layer, slot, chans)
    lines_out = tile_of(size_y)
    for row in range(0, size_y, lines_out):
        spot = pl.ds(row, lines_out)
        value = conv_lines([(layer, 0, tap(0, odd)), (layer, 1, tap(1, odd))], row, lines_out, weight_two)
        first = jnp.maximum(value + out_far[spot], 0.0).astype(BF16)
        skipped[odd, spot] = first
        value = conv_lines([(layer, 1, tap(0, odd))], row, lines_out, weight_two)
        second = jnp.maximum(value + out_near[spot], 0.0).astype(BF16)
        skipped[1 - odd, spot] = second
        both = first.astype(F32) + second.astype(F32)
        for group in range(sums.shape[0]):
            sums[group, spot] = both[:, :, group * LANES : (group + 1) * LANES]
    for row in range(size_y // 2):
        for group in range(sums.shape[0]):
            pairs = [
                sums[group, 2 * row + step, pl.ds(side, depth // 2, stride=2)] for step in range(2) for side in range(2)
            ]
            mean = (pairs[0] + pairs[1] + pairs[2] + pairs[3]) * 0.125
            pooled[row, :, group * LANES : (group + 1) * LANES] = mean.astype(BF16)


def kernel_c(*refs, chans):
    blocks = refs[: 3 * chans]
    weight, projection = refs[3 * chans : 3 * chans + 2]
    own_part, sent = refs[3 * chans + 2], refs[3 * chans + 3 : 4 * chans + 2]
    field, parts = refs[4 * chans + 2 :]
    odd = lax.rem(lax.axis_index("brick"), 2)
    chan = lax.axis_index("chan")
    rows, depth = blocks[0].shape[0], blocks[0].shape[1]
    total = chans * rows
    for plane in range(3):
        zeros = jnp.zeros(field.shape[2:], field.dtype)
        field[plane, 0] = zeros
        field[plane, total + 1] = zeros
        for step in range(chans):
            source = lax.rem(chan - step + chans, chans)
            field[plane, pl.ds(1 + source * rows, rows)] = blocks[plane * chans + step][...]
    lines = tile_of(total)
    for row in range(0, total, lines):
        value = conv_lines([(field, step, tap(step, odd)) for step in range(3)], row, lines, weight)
        value = jnp.maximum(value, 0.0).astype(BF16).reshape(lines * depth, weight.shape[4])
        part = jnp.dot(value, projection[...], preferred_element_type=F32)
        parts[pl.ds(row, lines)] = part.reshape(lines, depth, part.shape[1])
    own_part[...] = parts[pl.ds(chan * rows, rows)]
    for step in range(1, chans):
        target = lax.rem(chan + step, chans)
        sent[step - 1][...] = parts[pl.ds(target * rows, rows)].astype(BF16)


def kernel_d(*refs):
    skipped, own_part = refs[0], refs[1]
    received, merged, fine = refs[2:-2], refs[-2], refs[-1]
    rows, depth = own_part.shape[0], own_part.shape[1]
    lifted = own_part[...]
    for part in received:
        lifted = lifted + part[...].astype(F32)
    for group in range(fine.shape[0]):
        lanes = slice(group * LANES, (group + 1) * LANES)
        for row in range(rows):
            for side in range(2):
                fine[group, row, pl.ds(side, depth, stride=2)] = lifted[row, :, lanes]
        for row in range(rows):
            value = fine[group, row]
            for plane in range(2):
                for step in range(2):
                    line = 2 * row + step
                    merged[plane, line, :, lanes] = (skipped[plane, line, :, lanes].astype(F32) + value).astype(BF16)


def shards(volume, first_weight, second_weight, coarse_weight, projection):
    chans = lax.axis_size("chan")
    size_x, size_y, depth, channels = volume.shape
    assert size_x == 2 and lax.axis_size("brick") % 2 == 0

    turns_of_edges = [[], [lambda c: 1 - c]][chans - 1] if chans <= 2 else [lambda c: c + 1, lambda c: c - 1]
    edges = []
    if chans > 1:
        edges = call(
            functools.partial(send_edges, chans=chans),
            [volume],
            [((2, 2, depth, channels), BF16)] * len(turns_of_edges),
            [],
            WEIGHT_COPY_FLOPS,
            16,
        )
    far = exchange(volume, "far", lambda c: c)
    own_halos = [exchange(edge, "own", turn) for edge, turn in zip(edges, turns_of_edges)]
    far_halos = [exchange(edge, "far", turn) for edge, turn in zip(edges, turns_of_edges)]
    near = exchange(volume, "near", lambda c: c)
    near_halos = [exchange(halo, "near", lambda c: c) for halo in own_halos]

    rows = size_y + min(chans - 1, 2)
    flops_of_plane = 2 * size_y * depth * 9 * channels * channels
    static = dict(chans=chans, halo_count=len(edges))
    partials = call(
        functools.partial(kernel_a, **static),
        [volume, *own_halos, near, *near_halos, first_weight, second_weight],
        [((rows, depth, channels), F32)] * 2 + [((size_y, depth, channels), F32)] * 2,
        [pltpu.VMEM((4, size_y + 4, depth, channels), BF16), pltpu.VMEM((2, size_y + 2, depth, channels), BF16)],
        12 * flops_of_plane,
        16,
    )
    skipped, pooled = call(
        functools.partial(kernel_b, **static),
        [far, *far_halos, *partials, first_weight, second_weight],
        [(volume.shape, BF16), ((size_y // 2, depth // 2, channels), BF16)],
        [
            pltpu.VMEM((2, size_y + 4, depth, channels), BF16),
            pltpu.VMEM((2, size_y + 2, depth, channels), BF16),
            pltpu.VMEM((channels // LANES, size_y, depth, LANES), F32),
        ],
        6 * flops_of_plane,
        16,
    )

    turns = [(lambda c, step=step: (c + step) % chans) for step in range(chans)]
    own_blocks = [pooled] + [exchange(pooled, "own", turn) for turn in turns[1:]]
    far_blocks = [exchange(pooled, "far", turns[0])]
    far_blocks += [exchange(pooled, "far", turn) for turn in turns[1:]]
    near_blocks = [exchange(pooled, "near", turns[0])]
    near_blocks += [exchange(block, "near", turns[0]) for block in own_blocks[1:]]
    part_shape = (size_y // 2, depth // 2, channels)
    coarse_rows = chans * size_y // 2
    parts = call(
        functools.partial(kernel_c, chans=chans),
        [*far_blocks, *own_blocks, *near_blocks, coarse_weight, projection],
        [(part_shape, F32)] + [(part_shape, BF16)] * (chans - 1),
        [
            pltpu.VMEM((3, coarse_rows + 2, depth // 2, channels), BF16),
            pltpu.VMEM((coarse_rows, depth // 2, channels), F32),
        ],
        2 * coarse_rows * (depth // 2) * 27 * channels * coarse_weight.shape[4],
        16,
    )
    received = [exchange(part, "own", turn) for part, turn in zip(parts[1:], turns[1:])]
    return call(
        kernel_d,
        [skipped, parts[0], *received],
        [(volume.shape, BF16)],
        [pltpu.VMEM((channels // LANES, size_y // 2, depth, LANES), F32)],
        volume.size,
        16,
        results_in_vmem=False,
    )[0]


def solution(mesh):
    in_specs = (
        P("brick", "chan", None, None),
        P(),
        P(),
        P(None, None, None, None, "chan"),
        P("chan", None),
    )
    out_specs = P("brick", "chan", None, None)

    return jax.shard_map(shards, mesh=mesh, in_specs=in_specs, out_specs=out_specs, check_vma=False)
```

```python
import functools

import jax
import jax.numpy as jnp
from jax import lax
from jax.experimental import pallas as pl
from jax.experimental.pallas import tpu as pltpu
from jax.sharding import PartitionSpec as P


AXES = ("brick", "chan")
BF16 = jnp.bfloat16
F32 = jnp.float32
LANES = 128
WEIGHT_COPY_FLOPS = 2**33
VMEM_SPEC = pl.BlockSpec(memory_space=pltpu.VMEM)


def brick_partner(kind, brick, bricks):
    if kind == "own":
        return brick
    partner = brick ^ 1 if kind == "near" else ((brick + 1) ^ 1) - 1
    return partner if 0 <= partner < bricks else None


def exchange(value, kind, chan_of):
    bricks, chans = lax.axis_size("brick"), lax.axis_size("chan")
    pairs = []
    for brick in range(bricks):
        for chan in range(chans):
            other, target = brick_partner(kind, brick, bricks), chan_of(chan)
            if other is not None and target is not None and 0 <= target < chans:
                pairs.append((brick * chans + chan, other * chans + target))
    return lax.ppermute(value, AXES, pairs)


def row_split(chans, size_y):
    chan = lax.axis_index("chan")
    if chans == 1:
        return [], (0, size_y)
    if chans == 2:
        return [(jnp.where(chan == 0, size_y - 2, 0), 2)], (jnp.where(chan == 0, 0, 2), size_y - 2)
    return [(size_y - 2, 2), (0, 2)], (2, size_y - 4)


def early(out):
    out[...] = jnp.zeros_like(out)


def split_rows(volume, _, *pieces, chans):
    sides, rest = row_split(chans, volume.shape[1])
    for piece, (start, count) in zip(pieces, [*sides, rest]):
        piece[...] = volume[:, pl.ds(start, count)]


def call(kernel, inputs, outputs, scratch, flops, limit_mib, results_in_vmem=True):
    inputs = [pltpu.with_memory_space_constraint(value, pltpu.VMEM) for value in inputs]
    if results_in_vmem:
        out_shape = [pltpu.VMEM(shape, dtype) for shape, dtype in outputs]
    else:
        out_shape = [jax.ShapeDtypeStruct(shape, dtype) for shape, dtype in outputs]
    return pl.pallas_call(
        kernel,
        out_shape=out_shape,
        in_specs=[VMEM_SPEC] * len(inputs),
        out_specs=[VMEM_SPEC] * len(outputs),
        scratch_shapes=scratch,
        compiler_params=pltpu.CompilerParams(vmem_limit_bytes=limit_mib * 2**20),
        cost_estimate=pl.CostEstimate(flops=flops, bytes_accessed=2**20, transcendentals=0),
    )(*inputs)


def tile_of(rows):
    return max(lines for lines in range(1, 10) if rows % lines == 0)


def conv_lines(terms, row, lines, weight):
    sums = []
    for dz in range(3):
        total = None
        for ref, plane, dx in terms:
            for dy in range(3):
                window = ref[plane, pl.ds(row + dy, lines)]
                window = window.reshape(lines * window.shape[1], window.shape[2])
                part = jnp.dot(window, weight[dx, dy, dz], preferred_element_type=F32)
                total = part if total is None else total + part
        sums.append(total)
    depth = terms[0][0].shape[2]
    count = sums[0].shape[0]
    place = lax.rem(lax.broadcasted_iota(jnp.int32, sums[0].shape, 0), depth)
    before = jnp.where(place == 0, 0.0, pltpu.roll(sums[0], 1, 0))
    after = jnp.where(place == depth - 1, 0.0, pltpu.roll(sums[2], count - 1, 0))
    return (before + sums[1] + after).reshape(lines, depth, sums[0].shape[1])


def tap(step, odd):
    return step + odd * (2 - 2 * step)


def halo_plan(chans, size_y):
    chan = lax.axis_index("chan")
    if chans == 1:
        return []
    if chans == 2:
        return [(jnp.where(chan == 1, 0, size_y + 2), jnp.where(chan == 1, size_y + 2, 0))]
    return [(0, None), (size_y + 2, None)]


def fill_planes(target, slot, plane, pieces, halos, chans):
    size_y = target.shape[1] - 4
    for start, block in pieces:
        target[slot, pl.ds(start + 2, block.shape[1])] = block[plane]
    zeros = jnp.zeros((2,) + target.shape[2:], target.dtype)
    if chans == 1:
        target[slot, 0:2] = zeros
        target[slot, size_y + 2 : size_y + 4] = zeros
    for (place, empty), halo in zip(halo_plan(chans, size_y), halos):
        target[slot, pl.ds(place, 2)] = halo[plane]
        if empty is not None:
            target[slot, pl.ds(empty, 2)] = zeros


def first_row(chans):
    if chans == 1:
        return 0
    if chans == 2:
        return -lax.axis_index("chan")
    return -1


def clear_outside(layer, slot, chans):
    chan = lax.axis_index("chan")
    last = layer.shape[1] - 1
    for row, owner in ((0, 0), (last, chans - 1)):
        if chans <= 2:
            keep = jnp.logical_and(chans == 2, chan != owner)
        else:
            keep = chan != owner
        layer[slot, row] = jnp.where(keep, layer[slot, row], jnp.zeros_like(layer[slot, row]))


def kernel_a(*refs, chans, halo_count):
    own, own_halos = refs[0], refs[1 : 1 + halo_count]
    near, near_halos = refs[1 + halo_count], refs[2 + halo_count : 2 + 2 * halo_count]
    weight_one, weight_two, layer_far, layer_own, out_far, out_near, field, layer = refs[2 + 2 * halo_count :]
    odd = lax.rem(lax.axis_index("brick"), 2)
    size_y = own.shape[1]
    fill_planes(field, 0, odd, [(0, own)], own_halos, chans)
    fill_planes(field, 1, 1 - odd, [(0, own)], own_halos, chans)
    fill_planes(field, 2, odd, [(0, near)], near_halos, chans)
    fill_planes(field, 3, 1 - odd, [(0, near)], near_halos, chans)
    start = first_row(chans)
    rows = layer_far.shape[0]
    lines = tile_of(rows)
    for row in range(0, rows, lines):
        base = start + row + 1
        for slot in range(2):
            terms = [(field, slot + step, tap(step, odd)) for step in range(3)]
            value = jnp.maximum(conv_lines(terms, base, lines, weight_one), 0.0).astype(BF16)
            layer[slot, pl.ds(start + row + 1, lines)] = value
    for slot in range(2):
        clear_outside(layer, slot, chans)
    lines_out = tile_of(size_y)
    for row in range(0, size_y, lines_out):
        out_far[pl.ds(row, lines_out)] = conv_lines([(layer, 0, tap(2, odd))], row, lines_out, weight_two)
        out_near[pl.ds(row, lines_out)] = conv_lines(
            [(layer, 0, tap(1, odd)), (layer, 1, tap(2, odd))], row, lines_out, weight_two
        )
    for row in range(0, rows, lines):
        base = start + row + 1
        layer_own[pl.ds(row, lines)] = conv_lines(
            [(field, 0, tap(1, odd)), (field, 1, tap(2, odd))], base, lines, weight_one
        )
        layer_far[pl.ds(row, lines)] = conv_lines([(field, 0, tap(2, odd))], base, lines, weight_one)


def kernel_b(*refs, chans, halo_count):
    rest, edges, far_halos = refs[0], refs[1 : 1 + halo_count], refs[1 + halo_count : 1 + 2 * halo_count]
    layer_far, layer_own, out_far, out_near, weight_one, weight_two = refs[1 + 2 * halo_count : 7 + 2 * halo_count]
    skipped, pooled, field, layer, sums = refs[7 + 2 * halo_count :]
    brick = lax.axis_index("brick")
    odd = lax.rem(brick, 2)
    size_y, depth = out_far.shape[0], out_far.shape[1]
    sides, between = row_split(chans, size_y)
    far = [(start, edge) for (start, _), edge in zip(sides, edges)] + [(between[0], rest)]
    fill_planes(field, 0, odd, far, far_halos, chans)
    fill_planes(field, 1, 1 - odd, far, far_halos, chans)
    inside = jnp.logical_and(brick + odd > 0, brick + odd < lax.axis_size("brick"))
    start = first_row(chans)
    rows = layer_far.shape[0]
    lines = tile_of(rows)
    for row in range(0, rows, lines):
        base = start + row + 1
        value = conv_lines([(field, 0, tap(0, odd)), (field, 1, tap(1, odd))], base, lines, weight_one)
        value = jnp.maximum(value + layer_far[pl.ds(row, lines)], 0.0)
        layer[0, pl.ds(base, lines)] = jnp.where(inside, value, 0.0).astype(BF16)
        value = conv_lines([(field, 1, tap(0, odd))], base, lines, weight_one)
        value = jnp.maximum(value + layer_own[pl.ds(row, lines)], 0.0)
        layer[1, pl.ds(base, lines)] = value.astype(BF16)
    for slot in range(2):
        clear_outside(layer, slot, chans)
    lines_out = tile_of(size_y)
    for row in range(0, size_y, lines_out):
        spot = pl.ds(row, lines_out)
        value = conv_lines([(layer, 0, tap(0, odd)), (layer, 1, tap(1, odd))], row, lines_out, weight_two)
        first = jnp.maximum(value + out_far[spot], 0.0).astype(BF16)
        skipped[odd, spot] = first
        value = conv_lines([(layer, 1, tap(0, odd))], row, lines_out, weight_two)
        second = jnp.maximum(value + out_near[spot], 0.0).astype(BF16)
        skipped[1 - odd, spot] = second
        both = first.astype(F32) + second.astype(F32)
        for group in range(sums.shape[0]):
            sums[group, spot] = both[:, :, group * LANES : (group + 1) * LANES]
    for row in range(size_y // 2):
        for group in range(sums.shape[0]):
            pairs = [
                sums[group, 2 * row + step, pl.ds(side, depth // 2, stride=2)] for step in range(2) for side in range(2)
            ]
            mean = (pairs[0] + pairs[1] + pairs[2] + pairs[3]) * 0.125
            pooled[row, :, group * LANES : (group + 1) * LANES] = mean.astype(BF16)


def kernel_c(*refs, chans):
    blocks = refs[: 3 * chans]
    weight, projection = refs[3 * chans : 3 * chans + 2]
    own_part, sent = refs[3 * chans + 2], refs[3 * chans + 3 : 4 * chans + 2]
    field, parts = refs[4 * chans + 2 :]
    odd = lax.rem(lax.axis_index("brick"), 2)
    chan = lax.axis_index("chan")
    rows, depth = blocks[0].shape[0], blocks[0].shape[1]
    total = chans * rows
    for plane in range(3):
        zeros = jnp.zeros(field.shape[2:], field.dtype)
        field[plane, 0] = zeros
        field[plane, total + 1] = zeros
        for step in range(chans):
            source = lax.rem(chan - step + chans, chans)
            field[plane, pl.ds(1 + source * rows, rows)] = blocks[plane * chans + step][...]
    lines = tile_of(total)
    for row in range(0, total, lines):
        value = conv_lines([(field, step, tap(step, odd)) for step in range(3)], row, lines, weight)
        value = jnp.maximum(value, 0.0).astype(BF16).reshape(lines * depth, weight.shape[4])
        part = jnp.dot(value, projection[...], preferred_element_type=F32)
        parts[pl.ds(row, lines)] = part.reshape(lines, depth, part.shape[1])
    own_part[...] = parts[pl.ds(chan * rows, rows)]
    for step in range(1, chans):
        target = lax.rem(chan + step, chans)
        sent[step - 1][...] = parts[pl.ds(target * rows, rows)].astype(BF16)


def kernel_d(*refs):
    skipped, own_part = refs[0], refs[1]
    received, merged, fine = refs[2:-2], refs[-2], refs[-1]
    rows, depth = own_part.shape[0], own_part.shape[1]
    lifted = own_part[...]
    for part in received:
        lifted = lifted + part[...].astype(F32)
    for group in range(fine.shape[0]):
        lanes = slice(group * LANES, (group + 1) * LANES)
        for row in range(rows):
            for side in range(2):
                fine[group, row, pl.ds(side, depth, stride=2)] = lifted[row, :, lanes]
        for row in range(rows):
            value = fine[group, row]
            for plane in range(2):
                for step in range(2):
                    line = 2 * row + step
                    merged[plane, line, :, lanes] = (skipped[plane, line, :, lanes].astype(F32) + value).astype(BF16)


def shards(volume, first_weight, second_weight, coarse_weight, projection):
    chans = lax.axis_size("chan")
    size_x, size_y, depth, channels = volume.shape
    assert size_x == 2 and lax.axis_size("brick") % 2 == 0

    turns = [[], [lambda c: 1 - c]][chans - 1] if chans <= 2 else [lambda c: c + 1, lambda c: c - 1]
    same = lambda c: c
    near = exchange(volume, "near", same)
    token = call(early, [], [((8, LANES), F32)], [], WEIGHT_COPY_FLOPS, 4)[0]
    rest_rows = size_y - 2 * len(turns)
    *edges, rest = call(
        functools.partial(split_rows, chans=chans),
        [volume, token],
        [((2, 2, depth, channels), BF16)] * len(turns) + [((2, rest_rows, depth, channels), BF16)],
        [],
        WEIGHT_COPY_FLOPS,
        4,
    )
    own_halos = [exchange(edge, "own", turn) for edge, turn in zip(edges, turns)]
    far_edges = [exchange(edge, "far", same) for edge in edges]
    far_rest = exchange(rest, "far", same)
    near_halos = [exchange(halo, "near", same) for halo in own_halos]
    far_halos = [exchange(edge, "own", turn) for edge, turn in zip(far_edges, turns)]

    rows = size_y + min(chans - 1, 2)
    flops_of_plane = 2 * size_y * depth * 9 * channels * channels
    static = dict(chans=chans, halo_count=len(turns))
    partials = call(
        functools.partial(kernel_a, **static),
        [volume, *own_halos, near, *near_halos, first_weight, second_weight],
        [((rows, depth, channels), F32)] * 2 + [((size_y, depth, channels), F32)] * 2,
        [pltpu.VMEM((4, size_y + 4, depth, channels), BF16), pltpu.VMEM((2, size_y + 2, depth, channels), BF16)],
        12 * flops_of_plane,
        16,
    )
    skipped, pooled = call(
        functools.partial(kernel_b, **static),
        [far_rest, *far_edges, *far_halos, *partials, first_weight, second_weight],
        [(volume.shape, BF16), ((size_y // 2, depth // 2, channels), BF16)],
        [
            pltpu.VMEM((2, size_y + 4, depth, channels), BF16),
            pltpu.VMEM((2, size_y + 2, depth, channels), BF16),
            pltpu.VMEM((channels // LANES, size_y, depth, LANES), F32),
        ],
        6 * flops_of_plane,
        16,
    )

    turns = [(lambda c, step=step: (c + step) % chans) for step in range(chans)]
    own_blocks = [pooled] + [exchange(pooled, "own", turn) for turn in turns[1:]]
    far_blocks = [exchange(pooled, "far", turns[0])]
    far_blocks += [exchange(block, "far", turns[0]) for block in own_blocks[1:]]
    near_blocks = [exchange(pooled, "near", turns[0])]
    near_blocks += [exchange(block, "near", turns[0]) for block in own_blocks[1:]]
    part_shape = (size_y // 2, depth // 2, channels)
    coarse_rows = chans * size_y // 2
    parts = call(
        functools.partial(kernel_c, chans=chans),
        [*far_blocks, *own_blocks, *near_blocks, coarse_weight, projection],
        [(part_shape, F32)] + [(part_shape, BF16)] * (chans - 1),
        [
            pltpu.VMEM((3, coarse_rows + 2, depth // 2, channels), BF16),
            pltpu.VMEM((coarse_rows, depth // 2, channels), F32),
        ],
        2 * coarse_rows * (depth // 2) * 27 * channels * coarse_weight.shape[4],
        16,
    )
    received = [exchange(part, "own", turn) for part, turn in zip(parts[1:], turns[1:])]
    return call(
        kernel_d,
        [skipped, parts[0], *received],
        [(volume.shape, BF16)],
        [pltpu.VMEM((channels // LANES, size_y // 2, depth, LANES), F32)],
        volume.size,
        16,
        results_in_vmem=False,
    )[0]


def solution(mesh):
    in_specs = (
        P("brick", "chan", None, None),
        P(),
        P(),
        P(None, None, None, None, "chan"),
        P("chan", None),
    )
    out_specs = P("brick", "chan", None, None)

    return jax.shard_map(shards, mesh=mesh, in_specs=in_specs, out_specs=out_specs, check_vma=False)
```

```python
import functools

import jax
import jax.numpy as jnp
from jax import lax
from jax.experimental import pallas as pl
from jax.experimental.pallas import tpu as pltpu
from jax.sharding import PartitionSpec as P


AXES = ("brick", "chan")
BF16 = jnp.bfloat16
F32 = jnp.float32
LANES = 128
WEIGHT_COPY_FLOPS = 2**33
VMEM_SPEC = pl.BlockSpec(memory_space=pltpu.VMEM)


def brick_partner(kind, brick, bricks):
    if kind == "own":
        return brick
    partner = brick ^ 1 if kind == "near" else ((brick + 1) ^ 1) - 1
    return partner if 0 <= partner < bricks else None


def exchange(value, kind, chan_of=None):
    bricks, chans = lax.axis_size("brick"), lax.axis_size("chan")
    pairs = []
    for brick in range(bricks):
        for chan in range(chans):
            other = brick_partner(kind, brick, bricks)
            target = chan if chan_of is None else chan_of(chan)
            if other is None and chans % 2 == 0:
                other, target = brick, chan ^ 1
            if other is not None and 0 <= target < chans:
                pairs.append((brick * chans + chan, other * chans + target))
    return lax.ppermute(value, AXES, pairs)


def has_far():
    brick = lax.axis_index("brick")
    edge = brick + lax.rem(brick, 2)
    return jnp.logical_and(edge > 0, edge < lax.axis_size("brick"))


def row_split(chans, size_y):
    chan = lax.axis_index("chan")
    if chans == 1:
        return [], (0, size_y)
    if chans == 2:
        return [(jnp.where(chan == 0, size_y - 2, 0), 2)], (jnp.where(chan == 0, 0, 2), size_y - 2)
    return [(size_y - 2, 2), (0, 2)], (2, size_y - 4)


def early(out):
    out[...] = jnp.zeros_like(out)


def split_rows(volume, _, *pieces, chans):
    sides, rest = row_split(chans, volume.shape[1])
    for piece, (start, count) in zip(pieces, [*sides, rest]):
        piece[...] = volume[:, pl.ds(start, count)]


def call(kernel, inputs, outputs, scratch, flops, limit_mib, results_in_vmem=True):
    inputs = [pltpu.with_memory_space_constraint(value, pltpu.VMEM) for value in inputs]
    if results_in_vmem:
        out_shape = [pltpu.VMEM(shape, dtype) for shape, dtype in outputs]
    else:
        out_shape = [jax.ShapeDtypeStruct(shape, dtype) for shape, dtype in outputs]
    return pl.pallas_call(
        kernel,
        out_shape=out_shape,
        in_specs=[VMEM_SPEC] * len(inputs),
        out_specs=[VMEM_SPEC] * len(outputs),
        scratch_shapes=scratch,
        compiler_params=pltpu.CompilerParams(vmem_limit_bytes=limit_mib * 2**20),
        cost_estimate=pl.CostEstimate(flops=flops, bytes_accessed=2**20, transcendentals=0),
    )(*inputs)


def tile_of(rows):
    return max(lines for lines in range(1, 10) if rows % lines == 0)


def conv_lines(terms, row, lines, weight):
    sums = []
    for dz in range(3):
        total = None
        for ref, plane, dx in terms:
            for dy in range(3):
                window = ref[plane, pl.ds(row + dy, lines)]
                window = window.reshape(lines * window.shape[1], window.shape[2])
                part = jnp.dot(window, weight[dx, dy, dz], preferred_element_type=F32)
                total = part if total is None else total + part
        sums.append(total)
    depth = terms[0][0].shape[2]
    count = sums[0].shape[0]
    place = lax.rem(lax.broadcasted_iota(jnp.int32, sums[0].shape, 0), depth)
    before = jnp.where(place == 0, 0.0, pltpu.roll(sums[0], 1, 0))
    after = jnp.where(place == depth - 1, 0.0, pltpu.roll(sums[2], count - 1, 0))
    return (before + sums[1] + after).reshape(lines, depth, sums[0].shape[1])


def tap(step, odd):
    return step + odd * (2 - 2 * step)


def halo_plan(chans, size_y):
    chan = lax.axis_index("chan")
    if chans == 1:
        return []
    if chans == 2:
        return [(jnp.where(chan == 1, 0, size_y + 2), jnp.where(chan == 1, size_y + 2, 0))]
    return [(0, None), (size_y + 2, None)]


def fill_planes(target, slot, plane, pieces, halos, chans, valid=None):
    def rows_of(block):
        rows = block[plane]
        return rows if valid is None else jnp.where(valid, rows, jnp.zeros_like(rows))

    size_y = target.shape[1] - 4
    for start, block in pieces:
        target[slot, pl.ds(start + 2, block.shape[1])] = rows_of(block)
    zeros = jnp.zeros((2,) + target.shape[2:], target.dtype)
    if chans == 1:
        target[slot, 0:2] = zeros
        target[slot, size_y + 2 : size_y + 4] = zeros
    for (place, empty), halo in zip(halo_plan(chans, size_y), halos):
        target[slot, pl.ds(place, 2)] = rows_of(halo)
        if empty is not None:
            target[slot, pl.ds(empty, 2)] = zeros


def first_row(chans):
    if chans == 1:
        return 0
    if chans == 2:
        return -lax.axis_index("chan")
    return -1


def clear_outside(layer, slot, chans):
    chan = lax.axis_index("chan")
    last = layer.shape[1] - 1
    for row, owner in ((0, 0), (last, chans - 1)):
        if chans <= 2:
            keep = jnp.logical_and(chans == 2, chan != owner)
        else:
            keep = chan != owner
        layer[slot, row] = jnp.where(keep, layer[slot, row], jnp.zeros_like(layer[slot, row]))


def kernel_a(*refs, chans, halo_count):
    own, own_halos = refs[0], refs[1 : 1 + halo_count]
    near, near_halos = refs[1 + halo_count], refs[2 + halo_count : 2 + 2 * halo_count]
    weight_one, weight_two, layer_far, layer_own, out_far, out_near, field, layer = refs[2 + 2 * halo_count :]
    odd = lax.rem(lax.axis_index("brick"), 2)
    size_y = own.shape[1]
    fill_planes(field, 0, odd, [(0, own)], own_halos, chans)
    fill_planes(field, 1, 1 - odd, [(0, own)], own_halos, chans)
    fill_planes(field, 2, odd, [(0, near)], near_halos, chans)
    fill_planes(field, 3, 1 - odd, [(0, near)], near_halos, chans)
    start = first_row(chans)
    rows = layer_far.shape[0]
    lines = tile_of(rows)
    for row in range(0, rows, lines):
        base = start + row + 1
        for slot in range(2):
            terms = [(field, slot + step, tap(step, odd)) for step in range(3)]
            value = jnp.maximum(conv_lines(terms, base, lines, weight_one), 0.0).astype(BF16)
            layer[slot, pl.ds(start + row + 1, lines)] = value
    for slot in range(2):
        clear_outside(layer, slot, chans)
    lines_out = tile_of(size_y)
    for row in range(0, size_y, lines_out):
        out_far[pl.ds(row, lines_out)] = conv_lines([(layer, 0, tap(2, odd))], row, lines_out, weight_two)
        out_near[pl.ds(row, lines_out)] = conv_lines(
            [(layer, 0, tap(1, odd)), (layer, 1, tap(2, odd))], row, lines_out, weight_two
        )
    for row in range(0, rows, lines):
        base = start + row + 1
        layer_own[pl.ds(row, lines)] = conv_lines(
            [(field, 0, tap(1, odd)), (field, 1, tap(2, odd))], base, lines, weight_one
        )
        layer_far[pl.ds(row, lines)] = conv_lines([(field, 0, tap(2, odd))], base, lines, weight_one)


def kernel_b(*refs, chans, halo_count):
    rest, edges, far_halos = refs[0], refs[1 : 1 + halo_count], refs[1 + halo_count : 1 + 2 * halo_count]
    layer_far, layer_own, out_far, out_near, weight_one, weight_two = refs[1 + 2 * halo_count : 7 + 2 * halo_count]
    skipped, pooled, field, layer, sums = refs[7 + 2 * halo_count :]
    odd = lax.rem(lax.axis_index("brick"), 2)
    size_y, depth = out_far.shape[0], out_far.shape[1]
    sides, between = row_split(chans, size_y)
    far = [(start, edge) for (start, _), edge in zip(sides, edges)] + [(between[0], rest)]
    inside = has_far()
    fill_planes(field, 0, odd, far, far_halos, chans, inside)
    fill_planes(field, 1, 1 - odd, far, far_halos, chans, inside)
    start = first_row(chans)
    rows = layer_far.shape[0]
    lines = tile_of(rows)
    for row in range(0, rows, lines):
        base = start + row + 1
        value = conv_lines([(field, 0, tap(0, odd)), (field, 1, tap(1, odd))], base, lines, weight_one)
        value = jnp.maximum(value + layer_far[pl.ds(row, lines)], 0.0)
        layer[0, pl.ds(base, lines)] = jnp.where(inside, value, 0.0).astype(BF16)
        value = conv_lines([(field, 1, tap(0, odd))], base, lines, weight_one)
        value = jnp.maximum(value + layer_own[pl.ds(row, lines)], 0.0)
        layer[1, pl.ds(base, lines)] = value.astype(BF16)
    for slot in range(2):
        clear_outside(layer, slot, chans)
    lines_out = tile_of(size_y)
    for row in range(0, size_y, lines_out):
        spot = pl.ds(row, lines_out)
        value = conv_lines([(layer, 0, tap(0, odd)), (layer, 1, tap(1, odd))], row, lines_out, weight_two)
        first = jnp.maximum(value + out_far[spot], 0.0).astype(BF16)
        skipped[odd, spot] = first
        value = conv_lines([(layer, 1, tap(0, odd))], row, lines_out, weight_two)
        second = jnp.maximum(value + out_near[spot], 0.0).astype(BF16)
        skipped[1 - odd, spot] = second
        both = first.astype(F32) + second.astype(F32)
        for group in range(sums.shape[0]):
            sums[group, spot] = both[:, :, group * LANES : (group + 1) * LANES]
    for row in range(size_y // 2):
        for group in range(sums.shape[0]):
            pairs = [
                sums[group, 2 * row + step, pl.ds(side, depth // 2, stride=2)] for step in range(2) for side in range(2)
            ]
            mean = (pairs[0] + pairs[1] + pairs[2] + pairs[3]) * 0.125
            pooled[row, :, group * LANES : (group + 1) * LANES] = mean.astype(BF16)


def kernel_c(*refs, chans):
    blocks = refs[: 3 * chans]
    weight, projection = refs[3 * chans : 3 * chans + 2]
    own_part, sent = refs[3 * chans + 2], refs[3 * chans + 3 : 4 * chans + 2]
    field, parts = refs[4 * chans + 2 :]
    odd = lax.rem(lax.axis_index("brick"), 2)
    chan = lax.axis_index("chan")
    rows, depth = blocks[0].shape[0], blocks[0].shape[1]
    total = chans * rows
    inside = has_far()
    for plane in range(3):
        zeros = jnp.zeros(field.shape[2:], field.dtype)
        field[plane, 0] = zeros
        field[plane, total + 1] = zeros
        for step in range(chans):
            source = lax.rem(chan - step + chans, chans)
            block = blocks[plane * chans + step][...]
            if plane == 0:
                block = jnp.where(inside, block, jnp.zeros_like(block))
            field[plane, pl.ds(1 + source * rows, rows)] = block
    lines = tile_of(total)
    for row in range(0, total, lines):
        value = conv_lines([(field, step, tap(step, odd)) for step in range(3)], row, lines, weight)
        value = jnp.maximum(value, 0.0).astype(BF16).reshape(lines * depth, weight.shape[4])
        part = jnp.dot(value, projection[...], preferred_element_type=F32)
        parts[pl.ds(row, lines)] = part.reshape(lines, depth, part.shape[1])
    own_part[...] = parts[pl.ds(chan * rows, rows)]
    for step in range(1, chans):
        target = lax.rem(chan + step, chans)
        sent[step - 1][...] = parts[pl.ds(target * rows, rows)].astype(BF16)


def kernel_d(*refs):
    skipped, own_part = refs[0], refs[1]
    received, merged, fine = refs[2:-2], refs[-2], refs[-1]
    rows, depth = own_part.shape[0], own_part.shape[1]
    lifted = own_part[...]
    for part in received:
        lifted = lifted + part[...].astype(F32)
    for group in range(fine.shape[0]):
        lanes = slice(group * LANES, (group + 1) * LANES)
        for row in range(rows):
            for side in range(2):
                fine[group, row, pl.ds(side, depth, stride=2)] = lifted[row, :, lanes]
        for row in range(rows):
            value = fine[group, row]
            for plane in range(2):
                for step in range(2):
                    line = 2 * row + step
                    merged[plane, line, :, lanes] = (skipped[plane, line, :, lanes].astype(F32) + value).astype(BF16)


def shards(volume, first_weight, second_weight, coarse_weight, projection):
    chans = lax.axis_size("chan")
    size_x, size_y, depth, channels = volume.shape
    assert size_x == 2 and lax.axis_size("brick") % 2 == 0

    turns = [[], [lambda c: 1 - c]][chans - 1] if chans <= 2 else [lambda c: c + 1, lambda c: c - 1]
    near = exchange(volume, "near")
    token = call(early, [], [((8, LANES), F32)], [], WEIGHT_COPY_FLOPS, 4)[0]
    rest_rows = size_y - 2 * len(turns)
    *edges, rest = call(
        functools.partial(split_rows, chans=chans),
        [volume, token],
        [((2, 2, depth, channels), BF16)] * len(turns) + [((2, rest_rows, depth, channels), BF16)],
        [],
        WEIGHT_COPY_FLOPS,
        4,
    )
    own_halos = [exchange(edge, "own", turn) for edge, turn in zip(edges, turns)]
    far_edges = [exchange(edge, "far") for edge in edges]
    far_rest = exchange(rest, "far")
    near_halos = [exchange(halo, "near") for halo in own_halos]
    far_halos = [exchange(edge, "own", turn) for edge, turn in zip(far_edges, turns)]

    rows = size_y + min(chans - 1, 2)
    flops_of_plane = 2 * size_y * depth * 9 * channels * channels
    static = dict(chans=chans, halo_count=len(turns))
    partials = call(
        functools.partial(kernel_a, **static),
        [volume, *own_halos, near, *near_halos, first_weight, second_weight],
        [((rows, depth, channels), F32)] * 2 + [((size_y, depth, channels), F32)] * 2,
        [pltpu.VMEM((4, size_y + 4, depth, channels), BF16), pltpu.VMEM((2, size_y + 2, depth, channels), BF16)],
        12 * flops_of_plane,
        16,
    )
    skipped, pooled = call(
        functools.partial(kernel_b, **static),
        [far_rest, *far_edges, *far_halos, *partials, first_weight, second_weight],
        [(volume.shape, BF16), ((size_y // 2, depth // 2, channels), BF16)],
        [
            pltpu.VMEM((2, size_y + 4, depth, channels), BF16),
            pltpu.VMEM((2, size_y + 2, depth, channels), BF16),
            pltpu.VMEM((channels // LANES, size_y, depth, LANES), F32),
        ],
        6 * flops_of_plane,
        16,
    )

    turns = [(lambda c, step=step: (c + step) % chans) for step in range(chans)]
    own_blocks = [pooled] + [exchange(pooled, "own", turn) for turn in turns[1:]]
    far_blocks = [exchange(pooled, "far")]
    far_blocks += [exchange(block, "far") for block in own_blocks[1:]]
    near_blocks = [exchange(pooled, "near")]
    near_blocks += [exchange(block, "near") for block in own_blocks[1:]]
    part_shape = (size_y // 2, depth // 2, channels)
    coarse_rows = chans * size_y // 2
    parts = call(
        functools.partial(kernel_c, chans=chans),
        [*far_blocks, *own_blocks, *near_blocks, coarse_weight, projection],
        [(part_shape, F32)] + [(part_shape, BF16)] * (chans - 1),
        [
            pltpu.VMEM((3, coarse_rows + 2, depth // 2, channels), BF16),
            pltpu.VMEM((coarse_rows, depth // 2, channels), F32),
        ],
        2 * coarse_rows * (depth // 2) * 27 * channels * coarse_weight.shape[4],
        16,
    )
    received = [exchange(part, "own", turn) for part, turn in zip(parts[1:], turns[1:])]
    return call(
        kernel_d,
        [skipped, parts[0], *received],
        [(volume.shape, BF16)],
        [pltpu.VMEM((channels // LANES, size_y // 2, depth, LANES), F32)],
        volume.size,
        16,
        results_in_vmem=False,
    )[0]


def solution(mesh):
    in_specs = (
        P("brick", "chan", None, None),
        P(),
        P(),
        P(None, None, None, None, "chan"),
        P("chan", None),
    )
    out_specs = P("brick", "chan", None, None)

    return jax.shard_map(shards, mesh=mesh, in_specs=in_specs, out_specs=out_specs, check_vma=False)
```

```python
import functools

import jax
import jax.numpy as jnp
from jax import lax
from jax.experimental import pallas as pl
from jax.experimental.pallas import tpu as pltpu
from jax.sharding import PartitionSpec as P


AXES = ("brick", "chan")
BF16 = jnp.bfloat16
F32 = jnp.float32
LANES = 128
WEIGHT_COPY_FLOPS = 2**33
VMEM_SPEC = pl.BlockSpec(memory_space=pltpu.VMEM)


def brick_partner(kind, brick, bricks):
    if kind == "own":
        return brick
    partner = brick ^ 1 if kind == "near" else ((brick + 1) ^ 1) - 1
    return partner if 0 <= partner < bricks else None


def exchange(value, kind, chan_of=None):
    bricks, chans = lax.axis_size("brick"), lax.axis_size("chan")
    pairs = []
    for brick in range(bricks):
        for chan in range(chans):
            other = brick_partner(kind, brick, bricks)
            target = chan if chan_of is None else chan_of(chan)
            if other is None and chans % 2 == 0:
                other, target = brick, chan ^ 1
            if other is not None and 0 <= target < chans:
                pairs.append((brick * chans + chan, other * chans + target))
    return lax.ppermute(value, AXES, pairs)


def has_far():
    brick = lax.axis_index("brick")
    edge = brick + lax.rem(brick, 2)
    return jnp.logical_and(edge > 0, edge < lax.axis_size("brick"))


def early(out):
    out[...] = jnp.zeros_like(out)


def edge_rows(volume, _, *edges, chans):
    size_y = volume.shape[1]
    starts = [jnp.where(lax.axis_index("chan") == 0, size_y - 2, 0)] if chans == 2 else [size_y - 2, 0]
    for edge, start in zip(edges, starts):
        edge[...] = volume[:, pl.ds(start, 2)]


def call(kernel, inputs, outputs, scratch, flops, limit_mib, results_in_vmem=True):
    inputs = [pltpu.with_memory_space_constraint(value, pltpu.VMEM) for value in inputs]
    if results_in_vmem:
        out_shape = [pltpu.VMEM(shape, dtype) for shape, dtype in outputs]
    else:
        out_shape = [jax.ShapeDtypeStruct(shape, dtype) for shape, dtype in outputs]
    return pl.pallas_call(
        kernel,
        out_shape=out_shape,
        in_specs=[VMEM_SPEC] * len(inputs),
        out_specs=[VMEM_SPEC] * len(outputs),
        scratch_shapes=scratch,
        compiler_params=pltpu.CompilerParams(vmem_limit_bytes=limit_mib * 2**20),
        cost_estimate=pl.CostEstimate(flops=flops, bytes_accessed=2**20, transcendentals=0),
    )(*inputs)


def tile_of(rows):
    return max(lines for lines in range(1, 10) if rows % lines == 0)


def conv_lines(terms, row, lines, weight):
    sums = []
    for dz in range(3):
        total = None
        for ref, plane, dx in terms:
            for dy in range(3):
                window = ref[plane, pl.ds(row + dy, lines)]
                window = window.reshape(lines * window.shape[1], window.shape[2])
                part = jnp.dot(window, weight[dx, dy, dz], preferred_element_type=F32)
                total = part if total is None else total + part
        sums.append(total)
    depth = terms[0][0].shape[2]
    count = sums[0].shape[0]
    place = lax.rem(lax.broadcasted_iota(jnp.int32, sums[0].shape, 0), depth)
    before = jnp.where(place == 0, 0.0, pltpu.roll(sums[0], 1, 0))
    after = jnp.where(place == depth - 1, 0.0, pltpu.roll(sums[2], count - 1, 0))
    return (before + sums[1] + after).reshape(lines, depth, sums[0].shape[1])


def tap(step, odd):
    return step + odd * (2 - 2 * step)


def halo_plan(chans, size_y):
    chan = lax.axis_index("chan")
    if chans == 1:
        return []
    if chans == 2:
        return [(jnp.where(chan == 1, 0, size_y + 2), jnp.where(chan == 1, size_y + 2, 0))]
    return [(0, None), (size_y + 2, None)]


def fill_planes(target, slot, plane, block, halos, chans, valid=None):
    def rows_of(ref):
        rows = ref[plane]
        return rows if valid is None else jnp.where(valid, rows, jnp.zeros_like(rows))

    size_y = block.shape[1]
    target[slot, 2 : size_y + 2] = rows_of(block)
    zeros = jnp.zeros((2,) + target.shape[2:], target.dtype)
    if chans == 1:
        target[slot, 0:2] = zeros
        target[slot, size_y + 2 : size_y + 4] = zeros
    for (place, empty), halo in zip(halo_plan(chans, size_y), halos):
        target[slot, pl.ds(place, 2)] = rows_of(halo)
        if empty is not None:
            target[slot, pl.ds(empty, 2)] = zeros


def first_row(chans):
    if chans == 1:
        return 0
    if chans == 2:
        return -lax.axis_index("chan")
    return -1


def clear_outside(layer, slot, chans):
    chan = lax.axis_index("chan")
    last = layer.shape[1] - 1
    for row, owner in ((0, 0), (last, chans - 1)):
        if chans <= 2:
            keep = jnp.logical_and(chans == 2, chan != owner)
        else:
            keep = chan != owner
        layer[slot, row] = jnp.where(keep, layer[slot, row], jnp.zeros_like(layer[slot, row]))


def kernel_a(*refs, chans, halo_count):
    own, own_halos = refs[0], refs[1 : 1 + halo_count]
    near, near_halos = refs[1 + halo_count], refs[2 + halo_count : 2 + 2 * halo_count]
    weight_one, weight_two, layer_far, layer_own, out_far, out_near, field, layer = refs[2 + 2 * halo_count :]
    odd = lax.rem(lax.axis_index("brick"), 2)
    size_y = own.shape[1]
    fill_planes(field, 0, odd, own, own_halos, chans)
    fill_planes(field, 1, 1 - odd, own, own_halos, chans)
    fill_planes(field, 2, odd, near, near_halos, chans)
    fill_planes(field, 3, 1 - odd, near, near_halos, chans)
    start = first_row(chans)
    rows = layer_far.shape[0]
    lines = tile_of(rows)
    for row in range(0, rows, lines):
        base = start + row + 1
        for slot in range(2):
            terms = [(field, slot + step, tap(step, odd)) for step in range(3)]
            value = jnp.maximum(conv_lines(terms, base, lines, weight_one), 0.0).astype(BF16)
            layer[slot, pl.ds(start + row + 1, lines)] = value
    for slot in range(2):
        clear_outside(layer, slot, chans)
    lines_out = tile_of(size_y)
    for row in range(0, size_y, lines_out):
        out_far[pl.ds(row, lines_out)] = conv_lines([(layer, 0, tap(2, odd))], row, lines_out, weight_two)
        out_near[pl.ds(row, lines_out)] = conv_lines(
            [(layer, 0, tap(1, odd)), (layer, 1, tap(2, odd))], row, lines_out, weight_two
        )
    for row in range(0, rows, lines):
        base = start + row + 1
        layer_own[pl.ds(row, lines)] = conv_lines(
            [(field, 0, tap(1, odd)), (field, 1, tap(2, odd))], base, lines, weight_one
        )
        layer_far[pl.ds(row, lines)] = conv_lines([(field, 0, tap(2, odd))], base, lines, weight_one)


def kernel_b(*refs, chans, halo_count):
    far, far_halos = refs[0], refs[1 : 1 + halo_count]
    layer_far, layer_own, out_far, out_near, weight_one, weight_two = refs[1 + halo_count : 7 + halo_count]
    skipped, pooled, field, layer, sums = refs[7 + halo_count :]
    odd = lax.rem(lax.axis_index("brick"), 2)
    size_y, depth = out_far.shape[0], out_far.shape[1]
    inside = has_far()
    fill_planes(field, 0, odd, far, far_halos, chans, inside)
    fill_planes(field, 1, 1 - odd, far, far_halos, chans, inside)
    start = first_row(chans)
    rows = layer_far.shape[0]
    lines = tile_of(rows)
    for row in range(0, rows, lines):
        base = start + row + 1
        value = conv_lines([(field, 0, tap(0, odd)), (field, 1, tap(1, odd))], base, lines, weight_one)
        value = jnp.maximum(value + layer_far[pl.ds(row, lines)], 0.0)
        layer[0, pl.ds(base, lines)] = jnp.where(inside, value, 0.0).astype(BF16)
        value = conv_lines([(field, 1, tap(0, odd))], base, lines, weight_one)
        value = jnp.maximum(value + layer_own[pl.ds(row, lines)], 0.0)
        layer[1, pl.ds(base, lines)] = value.astype(BF16)
    for slot in range(2):
        clear_outside(layer, slot, chans)
    lines_out = tile_of(size_y)
    for row in range(0, size_y, lines_out):
        spot = pl.ds(row, lines_out)
        value = conv_lines([(layer, 0, tap(0, odd)), (layer, 1, tap(1, odd))], row, lines_out, weight_two)
        first = jnp.maximum(value + out_far[spot], 0.0).astype(BF16)
        skipped[odd, spot] = first
        value = conv_lines([(layer, 1, tap(0, odd))], row, lines_out, weight_two)
        second = jnp.maximum(value + out_near[spot], 0.0).astype(BF16)
        skipped[1 - odd, spot] = second
        both = first.astype(F32) + second.astype(F32)
        for group in range(sums.shape[0]):
            sums[group, spot] = both[:, :, group * LANES : (group + 1) * LANES]
    for row in range(size_y // 2):
        for group in range(sums.shape[0]):
            pairs = [
                sums[group, 2 * row + step, pl.ds(side, depth // 2, stride=2)] for step in range(2) for side in range(2)
            ]
            mean = (pairs[0] + pairs[1] + pairs[2] + pairs[3]) * 0.125
            pooled[row, :, group * LANES : (group + 1) * LANES] = mean.astype(BF16)


def kernel_c(*refs, chans):
    blocks = refs[: 3 * chans]
    weight, projection = refs[3 * chans : 3 * chans + 2]
    own_part, sent = refs[3 * chans + 2], refs[3 * chans + 3 : 4 * chans + 2]
    field, parts = refs[4 * chans + 2 :]
    odd = lax.rem(lax.axis_index("brick"), 2)
    chan = lax.axis_index("chan")
    rows, depth = blocks[0].shape[0], blocks[0].shape[1]
    total = chans * rows
    inside = has_far()
    for plane in range(3):
        zeros = jnp.zeros(field.shape[2:], field.dtype)
        field[plane, 0] = zeros
        field[plane, total + 1] = zeros
        for step in range(chans):
            source = lax.rem(chan - step + chans, chans)
            block = blocks[plane * chans + step][...]
            if plane == 0:
                block = jnp.where(inside, block, jnp.zeros_like(block))
            field[plane, pl.ds(1 + source * rows, rows)] = block
    lines = tile_of(total)
    for row in range(0, total, lines):
        value = conv_lines([(field, step, tap(step, odd)) for step in range(3)], row, lines, weight)
        value = jnp.maximum(value, 0.0).astype(BF16).reshape(lines * depth, weight.shape[4])
        part = jnp.dot(value, projection[...], preferred_element_type=F32)
        parts[pl.ds(row, lines)] = part.reshape(lines, depth, part.shape[1])
    own_part[...] = parts[pl.ds(chan * rows, rows)]
    for step in range(1, chans):
        target = lax.rem(chan + step, chans)
        sent[step - 1][...] = parts[pl.ds(target * rows, rows)].astype(BF16)


def kernel_d(*refs):
    skipped, own_part = refs[0], refs[1]
    received, merged, fine = refs[2:-2], refs[-2], refs[-1]
    rows, depth = own_part.shape[0], own_part.shape[1]
    lifted = own_part[...]
    for part in received:
        lifted = lifted + part[...].astype(F32)
    for group in range(fine.shape[0]):
        lanes = slice(group * LANES, (group + 1) * LANES)
        for row in range(rows):
            for side in range(2):
                fine[group, row, pl.ds(side, depth, stride=2)] = lifted[row, :, lanes]
        for row in range(rows):
            value = fine[group, row]
            for plane in range(2):
                for step in range(2):
                    line = 2 * row + step
                    merged[plane, line, :, lanes] = (skipped[plane, line, :, lanes].astype(F32) + value).astype(BF16)


def shards(volume, first_weight, second_weight, coarse_weight, projection):
    chans = lax.axis_size("chan")
    size_x, size_y, depth, channels = volume.shape
    assert size_x == 2 and lax.axis_size("brick") % 2 == 0

    turns = [[], [lambda c: 1 - c]][chans - 1] if chans <= 2 else [lambda c: c + 1, lambda c: c - 1]
    far = exchange(volume, "far")
    near = exchange(volume, "near")
    edges = []
    if chans > 1:
        token = call(early, [], [((8, LANES), F32)], [], WEIGHT_COPY_FLOPS, 4)[0]
        edges = call(
            functools.partial(edge_rows, chans=chans),
            [volume, token],
            [((2, 2, depth, channels), BF16)] * len(turns),
            [],
            WEIGHT_COPY_FLOPS,
            4,
        )
    own_halos = [exchange(edge, "own", turn) for edge, turn in zip(edges, turns)]
    far_halos = [exchange(halo, "far") for halo in own_halos]
    near_halos = [exchange(halo, "near") for halo in own_halos]

    rows = size_y + min(chans - 1, 2)
    flops_of_plane = 2 * size_y * depth * 9 * channels * channels
    static = dict(chans=chans, halo_count=len(turns))
    partials = call(
        functools.partial(kernel_a, **static),
        [volume, *own_halos, near, *near_halos, first_weight, second_weight],
        [((rows, depth, channels), F32)] * 2 + [((size_y, depth, channels), F32)] * 2,
        [pltpu.VMEM((4, size_y + 4, depth, channels), BF16), pltpu.VMEM((2, size_y + 2, depth, channels), BF16)],
        12 * flops_of_plane,
        16,
    )
    skipped, pooled = call(
        functools.partial(kernel_b, **static),
        [far, *far_halos, *partials, first_weight, second_weight],
        [(volume.shape, BF16), ((size_y // 2, depth // 2, channels), BF16)],
        [
            pltpu.VMEM((2, size_y + 4, depth, channels), BF16),
            pltpu.VMEM((2, size_y + 2, depth, channels), BF16),
            pltpu.VMEM((channels // LANES, size_y, depth, LANES), F32),
        ],
        6 * flops_of_plane,
        16,
    )

    turns = [(lambda c, step=step: (c + step) % chans) for step in range(chans)]
    own_blocks = [pooled] + [exchange(pooled, "own", turn) for turn in turns[1:]]
    far_blocks = [exchange(pooled, "far")]
    far_blocks += [exchange(block, "far") for block in own_blocks[1:]]
    near_blocks = [exchange(pooled, "near")]
    near_blocks += [exchange(block, "near") for block in own_blocks[1:]]
    part_shape = (size_y // 2, depth // 2, channels)
    coarse_rows = chans * size_y // 2
    parts = call(
        functools.partial(kernel_c, chans=chans),
        [*far_blocks, *own_blocks, *near_blocks, coarse_weight, projection],
        [(part_shape, F32)] + [(part_shape, BF16)] * (chans - 1),
        [
            pltpu.VMEM((3, coarse_rows + 2, depth // 2, channels), BF16),
            pltpu.VMEM((coarse_rows, depth // 2, channels), F32),
        ],
        2 * coarse_rows * (depth // 2) * 27 * channels * coarse_weight.shape[4],
        16,
    )
    received = [exchange(part, "own", turn) for part, turn in zip(parts[1:], turns[1:])]
    return call(
        kernel_d,
        [skipped, parts[0], *received],
        [(volume.shape, BF16)],
        [pltpu.VMEM((channels // LANES, size_y // 2, depth, LANES), F32)],
        volume.size,
        16,
        results_in_vmem=False,
    )[0]


def solution(mesh):
    in_specs = (
        P("brick", "chan", None, None),
        P(),
        P(),
        P(None, None, None, None, "chan"),
        P("chan", None),
    )
    out_specs = P("brick", "chan", None, None)

    return jax.shard_map(shards, mesh=mesh, in_specs=in_specs, out_specs=out_specs, check_vma=False)
```

```python
import functools

import jax
import jax.numpy as jnp
from jax import lax
from jax.experimental import pallas as pl
from jax.experimental.pallas import tpu as pltpu
from jax.sharding import PartitionSpec as P


AXES = ("brick", "chan")
BF16 = jnp.bfloat16
F32 = jnp.float32
LANES = 128
WEIGHT_COPY_FLOPS = 2**33
VMEM_SPEC = pl.BlockSpec(memory_space=pltpu.VMEM)


def brick_partner(kind, brick, bricks):
    if kind == "own":
        return brick
    partner = brick ^ 1 if kind == "near" else ((brick + 1) ^ 1) - 1
    return partner if 0 <= partner < bricks else None


def exchange(value, kind, chan_of=None):
    bricks, chans = lax.axis_size("brick"), lax.axis_size("chan")
    pairs = []
    for brick in range(bricks):
        for chan in range(chans):
            other = brick_partner(kind, brick, bricks)
            target = chan if chan_of is None else chan_of(chan)
            if other is None and chans % 2 == 0:
                other, target = brick, chan ^ 1
            if other is not None and 0 <= target < chans:
                pairs.append((brick * chans + chan, other * chans + target))
    return lax.ppermute(value, AXES, pairs)


def has_far():
    brick = lax.axis_index("brick")
    edge = brick + lax.rem(brick, 2)
    return jnp.logical_and(edge > 0, edge < lax.axis_size("brick"))


def early(out):
    out[...] = jnp.zeros_like(out)


def pieces_to_send(volume, _, first, second, *edges, chans):
    odd = lax.rem(lax.axis_index("brick"), 2)
    size_y = volume.shape[1]
    first[...] = volume[odd]
    second[...] = volume[1 - odd]
    starts = [jnp.where(lax.axis_index("chan") == 0, size_y - 2, 0)] if chans == 2 else [size_y - 2, 0]
    for edge, start in zip(edges, starts):
        edge[...] = volume[:, pl.ds(start, 2)]


def call(kernel, inputs, outputs, scratch, flops, limit_mib, results_in_vmem=True):
    inputs = [pltpu.with_memory_space_constraint(value, pltpu.VMEM) for value in inputs]
    if results_in_vmem:
        out_shape = [pltpu.VMEM(shape, dtype) for shape, dtype in outputs]
    else:
        out_shape = [jax.ShapeDtypeStruct(shape, dtype) for shape, dtype in outputs]
    return pl.pallas_call(
        kernel,
        out_shape=out_shape,
        in_specs=[VMEM_SPEC] * len(inputs),
        out_specs=[VMEM_SPEC] * len(outputs),
        scratch_shapes=scratch,
        compiler_params=pltpu.CompilerParams(vmem_limit_bytes=limit_mib * 2**20),
        cost_estimate=pl.CostEstimate(flops=flops, bytes_accessed=2**20, transcendentals=0),
    )(*inputs)


def tile_of(rows):
    return max(lines for lines in range(1, 10) if rows % lines == 0)


def conv_lines(terms, row, lines, weight):
    sums = []
    for dz in range(3):
        total = None
        for ref, plane, dx in terms:
            for dy in range(3):
                window = ref[plane, pl.ds(row + dy, lines)]
                window = window.reshape(lines * window.shape[1], window.shape[2])
                part = jnp.dot(window, weight[dx, dy, dz], preferred_element_type=F32)
                total = part if total is None else total + part
        sums.append(total)
    depth = terms[0][0].shape[2]
    count = sums[0].shape[0]
    place = lax.rem(lax.broadcasted_iota(jnp.int32, sums[0].shape, 0), depth)
    before = jnp.where(place == 0, 0.0, pltpu.roll(sums[0], 1, 0))
    after = jnp.where(place == depth - 1, 0.0, pltpu.roll(sums[2], count - 1, 0))
    return (before + sums[1] + after).reshape(lines, depth, sums[0].shape[1])


def tap(step, odd):
    return step + odd * (2 - 2 * step)


def halo_plan(chans, size_y):
    chan = lax.axis_index("chan")
    if chans == 1:
        return []
    if chans == 2:
        return [(jnp.where(chan == 1, 0, size_y + 2), jnp.where(chan == 1, size_y + 2, 0))]
    return [(0, None), (size_y + 2, None)]


def inner_rows(chans, size_y):
    return {1: (0, size_y), 2: (lax.axis_index("chan"), size_y - 1)}.get(chans, (1, size_y - 2))


def border_rows(chans, size_y):
    if chans == 1:
        return []
    if chans == 2:
        return [(jnp.where(lax.axis_index("chan") == 0, size_y - 1, -1), 2)]
    return [(-1, 2), (size_y - 1, 2)]


def row_groups(chans, size_y):
    return [inner_rows(chans, size_y), *border_rows(chans, size_y)]


def fill_plane(target, block, plane, halos, chans):
    valid = has_far()

    def masked(rows):
        return jnp.where(valid, rows, jnp.zeros_like(rows))

    size_y = block.shape[0]
    target[0, 2 : size_y + 2] = masked(block[...])
    zeros = jnp.zeros((2,) + target.shape[2:], target.dtype)
    if chans == 1:
        target[0, 0:2] = zeros
        target[0, size_y + 2 : size_y + 4] = zeros
    for (place, empty), halo in zip(halo_plan(chans, size_y), halos):
        target[0, pl.ds(place, 2)] = masked(halo[plane])
        if empty is not None:
            target[0, pl.ds(empty, 2)] = zeros


def clear_outside(layer, slot, chans):
    chan = lax.axis_index("chan")
    last = layer.shape[1] - 1
    for row, owner in ((0, 0), (last, chans - 1)):
        if chans <= 2:
            keep = jnp.logical_and(chans == 2, chan != owner)
        else:
            keep = chan != owner
        layer[slot, row] = jnp.where(keep, layer[slot, row], jnp.zeros_like(layer[slot, row]))


def kernel_a0(own, near, weight_one, done_three, done_four, part_one, part_two, field, *, chans):
    odd = lax.rem(lax.axis_index("brick"), 2)
    size_y = own.shape[1]
    zeros = jnp.zeros(field.shape[2:], field.dtype)
    for slot, (block, plane) in enumerate(((own, odd), (own, 1 - odd), (near, odd), (near, 1 - odd))):
        field[slot, 0] = zeros
        field[slot, 1 : size_y + 1] = block[plane]
        field[slot, size_y + 1] = zeros
    first, rows = inner_rows(chans, size_y)
    lines = tile_of(rows)
    for row in range(0, rows, lines):
        spot, base = pl.ds(row, lines), first + row
        for slot, done in enumerate((done_three, done_four)):
            terms = [(field, slot + step, tap(step, odd)) for step in range(3)]
            done[spot] = jnp.maximum(conv_lines(terms, base, lines, weight_one), 0.0).astype(BF16)
        terms = [(field, 0, tap(1, odd)), (field, 1, tap(2, odd))]
        part_two[spot] = conv_lines(terms, base, lines, weight_one)
        part_one[spot] = conv_lines([(field, 0, tap(2, odd))], base, lines, weight_one)


def kernel_a1(*refs, chans, sides):
    own, own_halos = refs[0], refs[1 : 1 + sides]
    near, near_halos = refs[1 + sides], refs[2 + sides : 2 + 2 * sides]
    done_three, done_four, weight_one, weight_two = refs[2 + 2 * sides : 6 + 2 * sides]
    out_two, out_three = refs[6 + 2 * sides : 8 + 2 * sides]
    parts = refs[8 + 2 * sides : 8 + 4 * sides]
    field, layer = refs[8 + 4 * sides :]
    odd = lax.rem(lax.axis_index("brick"), 2)
    size_y = own.shape[1]
    first, rows = inner_rows(chans, size_y)
    layer[0, pl.ds(first + 1, rows)] = done_three[...]
    layer[1, pl.ds(first + 1, rows)] = done_four[...]
    for side, (start, count) in enumerate(border_rows(chans, size_y)):
        high = start > 0
        place, source = jnp.where(high, 0, 2), jnp.where(high, size_y - 2, 0)
        planes = ((own, own_halos, odd), (own, own_halos, 1 - odd), (near, near_halos, odd), (near, near_halos, 1 - odd))
        for slot, (block, halos, plane) in enumerate(planes):
            field[slot, pl.ds(place, 2)] = block[plane, pl.ds(source, 2)]
            field[slot, pl.ds(2 - place, 2)] = halos[side][plane]
        for slot in range(2):
            terms = [(field, slot + step, tap(step, odd)) for step in range(3)]
            value = jnp.maximum(conv_lines(terms, 0, count, weight_one), 0.0).astype(BF16)
            layer[slot, pl.ds(start + 1, count)] = value
        terms = [(field, 0, tap(1, odd)), (field, 1, tap(2, odd))]
        parts[sides + side][...] = conv_lines(terms, 0, count, weight_one)
        parts[side][...] = conv_lines([(field, 0, tap(2, odd))], 0, count, weight_one)
    for slot in range(2):
        clear_outside(layer, slot, chans)
    lines = tile_of(size_y)
    for row in range(0, size_y, lines):
        spot = pl.ds(row, lines)
        out_two[spot] = conv_lines([(layer, 0, tap(2, odd))], row, lines, weight_two)
        out_three[spot] = conv_lines([(layer, 0, tap(1, odd)), (layer, 1, tap(2, odd))], row, lines, weight_two)


def kernel_b1(*refs, chans, sides):
    block, halos, refs = refs[0], refs[1 : 1 + sides], refs[1 + sides :]
    part_one, part_two, out_two, out_three, weight_one, weight_two = refs[0], refs[1], *refs[2 + 2 * sides : 6 + 2 * sides]
    ones, twos = [part_one, *refs[2 : 2 + sides]], [part_two, *refs[2 + sides : 2 + 2 * sides]]
    refs = refs[6 + 2 * sides :]
    skipped, more_two, mores = refs[0], refs[1], refs[2 : 3 + sides]
    field, layer = refs[3 + sides :]
    odd = lax.rem(lax.axis_index("brick"), 2)
    size_y = block.shape[0]
    fill_plane(field, block, 1 - odd, halos, chans)
    for (start, rows), one, two, more in zip(row_groups(chans, size_y), ones, twos, mores):
        lines = tile_of(rows)
        for row in range(0, rows, lines):
            spot, base = pl.ds(row, lines), start + row + 1
            value = conv_lines([(field, 0, tap(0, odd))], base, lines, weight_one)
            layer[0, pl.ds(base, lines)] = jnp.maximum(value + two[spot], 0.0).astype(BF16)
            more[spot] = one[spot] + conv_lines([(field, 0, tap(1, odd))], base, lines, weight_one)
    clear_outside(layer, 0, chans)
    lines = tile_of(size_y)
    for row in range(0, size_y, lines):
        spot = pl.ds(row, lines)
        value = conv_lines([(layer, 0, tap(0, odd))], row, lines, weight_two)
        skipped[spot] = jnp.maximum(value + out_three[spot], 0.0).astype(BF16)
        more_two[spot] = out_two[spot] + conv_lines([(layer, 0, tap(1, odd))], row, lines, weight_two)


def kernel_b2(*refs, chans, sides):
    block, halos, refs = refs[0], refs[1 : 1 + sides], refs[1 + sides :]
    other, out_two, mores, weight_one, weight_two = refs[0], refs[1], refs[2 : 3 + sides], *refs[3 + sides : 5 + sides]
    skipped, pooled, field, layer, sums = refs[5 + sides :]
    odd = lax.rem(lax.axis_index("brick"), 2)
    inside = has_far()
    size_y, depth = block.shape[0], block.shape[1]
    fill_plane(field, block, odd, halos, chans)
    for (start, rows), more in zip(row_groups(chans, size_y), mores):
        lines = tile_of(rows)
        for row in range(0, rows, lines):
            base = start + row + 1
            value = conv_lines([(field, 0, tap(0, odd))], base, lines, weight_one)
            value = jnp.maximum(value + more[pl.ds(row, lines)], 0.0)
            layer[0, pl.ds(base, lines)] = jnp.where(inside, value, 0.0).astype(BF16)
    clear_outside(layer, 0, chans)
    lines = tile_of(size_y)
    for row in range(0, size_y, lines):
        spot = pl.ds(row, lines)
        value = conv_lines([(layer, 0, tap(0, odd))], row, lines, weight_two)
        value = jnp.maximum(value + out_two[spot], 0.0).astype(BF16)
        skipped[spot] = value
        both = value.astype(F32) + other[spot].astype(F32)
        for group in range(sums.shape[0]):
            sums[group, spot] = both[:, :, group * LANES : (group + 1) * LANES]
    for row in range(size_y // 2):
        for group in range(sums.shape[0]):
            pairs = [
                sums[group, 2 * row + step, pl.ds(side, depth // 2, stride=2)] for step in range(2) for side in range(2)
            ]
            mean = (pairs[0] + pairs[1] + pairs[2] + pairs[3]) * 0.125
            pooled[row, :, group * LANES : (group + 1) * LANES] = mean.astype(BF16)


def kernel_c(*refs, chans):
    blocks = refs[: 3 * chans]
    weight, projection = refs[3 * chans : 3 * chans + 2]
    own_part, sent = refs[3 * chans + 2], refs[3 * chans + 3 : 4 * chans + 2]
    field, parts = refs[4 * chans + 2 :]
    odd = lax.rem(lax.axis_index("brick"), 2)
    chan = lax.axis_index("chan")
    rows, depth = blocks[0].shape[0], blocks[0].shape[1]
    total = chans * rows
    inside = has_far()
    for plane in range(3):
        zeros = jnp.zeros(field.shape[2:], field.dtype)
        field[plane, 0] = zeros
        field[plane, total + 1] = zeros
        for step in range(chans):
            source = lax.rem(chan - step + chans, chans)
            block = blocks[plane * chans + step][...]
            if plane == 0:
                block = jnp.where(inside, block, jnp.zeros_like(block))
            field[plane, pl.ds(1 + source * rows, rows)] = block
    lines = tile_of(total)
    for row in range(0, total, lines):
        value = conv_lines([(field, step, tap(step, odd)) for step in range(3)], row, lines, weight)
        value = jnp.maximum(value, 0.0).astype(BF16).reshape(lines * depth, weight.shape[4])
        part = jnp.dot(value, projection[...], preferred_element_type=F32)
        parts[pl.ds(row, lines)] = part.reshape(lines, depth, part.shape[1])
    own_part[...] = parts[pl.ds(chan * rows, rows)]
    for step in range(1, chans):
        target = lax.rem(chan + step, chans)
        sent[step - 1][...] = parts[pl.ds(target * rows, rows)].astype(BF16)


def kernel_d(*refs):
    skipped_two, skipped_three, own_part = refs[:3]
    received, merged, fine = refs[3:-2], refs[-2], refs[-1]
    odd = lax.rem(lax.axis_index("brick"), 2)
    rows, depth = own_part.shape[0], own_part.shape[1]
    lifted = own_part[...]
    for part in received:
        lifted = lifted + part[...].astype(F32)
    for group in range(fine.shape[0]):
        lanes = slice(group * LANES, (group + 1) * LANES)
        for row in range(rows):
            for side in range(2):
                fine[group, row, pl.ds(side, depth, stride=2)] = lifted[row, :, lanes]
        for row in range(rows):
            value = fine[group, row]
            for plane, skipped in ((odd, skipped_two), (1 - odd, skipped_three)):
                for step in range(2):
                    line = 2 * row + step
                    merged[plane, line, :, lanes] = (skipped[line, :, lanes].astype(F32) + value).astype(BF16)


def shards(volume, first_weight, second_weight, coarse_weight, projection):
    chans = lax.axis_size("chan")
    size_x, size_y, depth, channels = volume.shape
    assert size_x == 2 and lax.axis_size("brick") % 2 == 0

    turns = [[], [lambda c: 1 - c]][chans - 1] if chans <= 2 else [lambda c: c + 1, lambda c: c - 1]
    near = exchange(volume, "near")
    token = call(early, [], [((8, LANES), F32)], [], WEIGHT_COPY_FLOPS, 4)[0]
    plane_shape, sides = (size_y, depth, channels), len(turns)
    first, second, *edges = call(
        functools.partial(pieces_to_send, chans=chans),
        [volume, token],
        [(plane_shape, BF16)] * 2 + [((2, 2, depth, channels), BF16)] * sides,
        [],
        WEIGHT_COPY_FLOPS,
        4,
    )
    own_halos = [exchange(edge, "own", turn) for edge, turn in zip(edges, turns)]
    far_one = exchange(first, "far")
    far_halos = [exchange(halo, "far") for halo in own_halos]
    far_zero = exchange(second, "far")
    near_halos = [exchange(halo, "near") for halo in own_halos]

    static = dict(chans=chans, sides=sides)
    inner = inner_rows(chans, size_y)[1]
    border_shape = (2, depth, channels)
    line_flops = 2 * depth * 9 * channels * channels
    field_of_plane = pltpu.VMEM((1, size_y + 4, depth, channels), BF16)
    layer_of_plane = pltpu.VMEM((1, size_y + 2, depth, channels), BF16)
    done_three, done_four, part_one, part_two = call(
        functools.partial(kernel_a0, chans=chans),
        [volume, near, first_weight],
        [((inner, depth, channels), BF16)] * 2 + [((inner, depth, channels), F32)] * 2,
        [pltpu.VMEM((4, size_y + 2, depth, channels), BF16)],
        9 * inner * line_flops,
        12,
    )
    out_two, out_three, *border = call(
        functools.partial(kernel_a1, **static),
        [volume, *own_halos, near, *near_halos, done_three, done_four, first_weight, second_weight],
        [(plane_shape, F32)] * 2 + [(border_shape, F32)] * (2 * sides),
        [pltpu.VMEM((4, 4, depth, channels), BF16), pltpu.VMEM((2, size_y + 2, depth, channels), BF16)],
        (18 * sides + 3 * size_y) * line_flops,
        12,
    )
    skipped_three, out_two, *mores = call(
        functools.partial(kernel_b1, **static),
        [far_one, *far_halos, part_one, part_two, *border, out_two, out_three, first_weight, second_weight],
        [(plane_shape, BF16), (plane_shape, F32), ((inner, depth, channels), F32)] + [(border_shape, F32)] * sides,
        [field_of_plane, layer_of_plane],
        4 * size_y * line_flops,
        12,
    )
    skipped_two, pooled = call(
        functools.partial(kernel_b2, **static),
        [far_zero, *far_halos, skipped_three, out_two, *mores, first_weight, second_weight],
        [(plane_shape, BF16), ((size_y // 2, depth // 2, channels), BF16)],
        [field_of_plane, layer_of_plane, pltpu.VMEM((channels // LANES, size_y, depth, LANES), F32)],
        2 * size_y * line_flops,
        12,
    )

    turns = [(lambda c, step=step: (c + step) % chans) for step in range(chans)]
    own_blocks = [pooled] + [exchange(pooled, "own", turn) for turn in turns[1:]]
    far_blocks = [exchange(pooled, "far", turn) for turn in turns[1:]]
    far_blocks = [exchange(pooled, "far")] + far_blocks
    near_blocks = [exchange(pooled, "near")]
    near_blocks += [exchange(block, "near") for block in own_blocks[1:]]
    part_shape = (size_y // 2, depth // 2, channels)
    coarse_rows = chans * size_y // 2
    parts = call(
        functools.partial(kernel_c, chans=chans),
        [*far_blocks, *own_blocks, *near_blocks, coarse_weight, projection],
        [(part_shape, F32)] + [(part_shape, BF16)] * (chans - 1),
        [
            pltpu.VMEM((3, coarse_rows + 2, depth // 2, channels), BF16),
            pltpu.VMEM((coarse_rows, depth // 2, channels), F32),
        ],
        2 * coarse_rows * (depth // 2) * 27 * channels * coarse_weight.shape[4],
        16,
    )
    received = [exchange(part, "own", turn) for part, turn in zip(parts[1:], turns[1:])]
    return call(
        kernel_d,
        [skipped_two, skipped_three, parts[0], *received],
        [(volume.shape, BF16)],
        [pltpu.VMEM((channels // LANES, size_y // 2, depth, LANES), F32)],
        volume.size,
        16,
        results_in_vmem=False,
    )[0]


def solution(mesh):
    in_specs = (
        P("brick", "chan", None, None),
        P(),
        P(),
        P(None, None, None, None, "chan"),
        P("chan", None),
    )
    out_specs = P("brick", "chan", None, None)

    return jax.shard_map(shards, mesh=mesh, in_specs=in_specs, out_specs=out_specs, check_vma=False)
```

```python
import functools

import jax
import jax.numpy as jnp
from jax import lax
from jax.experimental import pallas as pl
from jax.experimental.pallas import tpu as pltpu
from jax.sharding import PartitionSpec as P


AXES = ("brick", "chan")
BF16 = jnp.bfloat16
F32 = jnp.float32
LANES = 128
WEIGHT_COPY_FLOPS = 2**33
VMEM_SPEC = pl.BlockSpec(memory_space=pltpu.VMEM)


def brick_partner(kind, brick, bricks):
    if kind == "own":
        return brick
    partner = brick ^ 1 if kind == "near" else ((brick + 1) ^ 1) - 1
    return partner if 0 <= partner < bricks else None


def exchange(value, kind, chan_of=None):
    bricks, chans = lax.axis_size("brick"), lax.axis_size("chan")
    pairs = []
    for brick in range(bricks):
        for chan in range(chans):
            other = brick_partner(kind, brick, bricks)
            target = chan if chan_of is None else chan_of(chan)
            if other is None and chans % 2 == 0:
                other, target = brick, chan ^ 1
            if other is not None and 0 <= target < chans:
                pairs.append((brick * chans + chan, other * chans + target))
    return lax.ppermute(value, AXES, pairs)


def has_far():
    brick = lax.axis_index("brick")
    edge = brick + lax.rem(brick, 2)
    return jnp.logical_and(edge > 0, edge < lax.axis_size("brick"))


def early(out):
    out[...] = jnp.zeros_like(out)


def pieces_to_send(volume, _, first, second, *edges, chans):
    odd = lax.rem(lax.axis_index("brick"), 2)
    size_y = volume.shape[1]
    first[...] = volume[odd]
    second[...] = volume[1 - odd]
    starts = [jnp.where(lax.axis_index("chan") == 0, size_y - 2, 0)] if chans == 2 else [size_y - 2, 0]
    for edge, start in zip(edges, starts):
        edge[...] = volume[:, pl.ds(start, 2)]


def call(kernel, inputs, outputs, scratch, flops, limit_mib, results_in_vmem=True):
    inputs = [pltpu.with_memory_space_constraint(value, pltpu.VMEM) for value in inputs]
    if results_in_vmem:
        out_shape = [pltpu.VMEM(shape, dtype) for shape, dtype in outputs]
    else:
        out_shape = [jax.ShapeDtypeStruct(shape, dtype) for shape, dtype in outputs]
    return pl.pallas_call(
        kernel,
        out_shape=out_shape,
        in_specs=[VMEM_SPEC] * len(inputs),
        out_specs=[VMEM_SPEC] * len(outputs),
        scratch_shapes=scratch,
        compiler_params=pltpu.CompilerParams(vmem_limit_bytes=limit_mib * 2**20),
        cost_estimate=pl.CostEstimate(flops=flops, bytes_accessed=2**20, transcendentals=0),
    )(*inputs)


def tile_of(rows):
    return max(lines for lines in range(1, 10) if rows % lines == 0)


def conv_lines(terms, row, lines, weight):
    sums = []
    for dz in range(3):
        total = None
        for ref, plane, dx in terms:
            for dy in range(3):
                window = ref[plane, pl.ds(row + dy, lines)]
                window = window.reshape(lines * window.shape[1], window.shape[2])
                part = jnp.dot(window, weight[dx, dy, dz], preferred_element_type=F32)
                total = part if total is None else total + part
        sums.append(total)
    depth = terms[0][0].shape[2]
    count = sums[0].shape[0]
    place = lax.rem(lax.broadcasted_iota(jnp.int32, sums[0].shape, 0), depth)
    before = jnp.where(place == 0, 0.0, pltpu.roll(sums[0], 1, 0))
    after = jnp.where(place == depth - 1, 0.0, pltpu.roll(sums[2], count - 1, 0))
    return (before + sums[1] + after).reshape(lines, depth, sums[0].shape[1])


def tap(step, odd):
    return step + odd * (2 - 2 * step)


def inner_rows(chans, size_y):
    return {1: (0, size_y), 2: (lax.axis_index("chan"), size_y - 1)}.get(chans, (1, size_y - 2))


def border_rows(chans, size_y):
    if chans == 1:
        return []
    if chans == 2:
        return [(jnp.where(lax.axis_index("chan") == 0, size_y - 1, -1), 2)]
    return [(-1, 2), (size_y - 1, 2)]


def fill_inner(target, planes, valid=None):
    size_y = target.shape[1] - 2
    zeros = jnp.zeros(target.shape[2:], target.dtype)
    for slot, (block, plane) in enumerate(planes):
        rows = block[...] if plane is None else block[plane]
        target[slot, 0] = zeros
        target[slot, 1 : size_y + 1] = rows if valid is None else jnp.where(valid, rows, jnp.zeros_like(rows))
        target[slot, size_y + 1] = zeros


def fill_border(target, start, size_y, planes, valid=None):
    high = start > 0
    place, source = jnp.where(high, 0, 2), jnp.where(high, size_y - 2, 0)
    for slot, (block, plane, halo, halo_plane) in enumerate(planes):
        rows = block[pl.ds(source, 2)] if plane is None else block[plane, pl.ds(source, 2)]
        beyond = halo[halo_plane]
        if valid is not None:
            rows = jnp.where(valid, rows, jnp.zeros_like(rows))
            beyond = jnp.where(valid, beyond, jnp.zeros_like(beyond))
        target[slot, pl.ds(place, 2)] = rows
        target[slot, pl.ds(2 - place, 2)] = beyond


def clear_outside(layer, slot, chans):
    chan = lax.axis_index("chan")
    last = layer.shape[1] - 1
    for row, owner in ((0, 0), (last, chans - 1)):
        if chans <= 2:
            keep = jnp.logical_and(chans == 2, chan != owner)
        else:
            keep = chan != owner
        layer[slot, row] = jnp.where(keep, layer[slot, row], jnp.zeros_like(layer[slot, row]))


def kernel_a0(own, near, weight_one, done_three, done_four, part_one, part_two, field, *, chans):
    odd = lax.rem(lax.axis_index("brick"), 2)
    size_y = own.shape[1]
    fill_inner(field, ((own, odd), (own, 1 - odd), (near, odd), (near, 1 - odd)))
    first, rows = inner_rows(chans, size_y)
    lines = tile_of(rows)
    for row in range(0, rows, lines):
        spot, base = pl.ds(row, lines), first + row
        for slot, done in enumerate((done_three, done_four)):
            terms = [(field, slot + step, tap(step, odd)) for step in range(3)]
            done[spot] = jnp.maximum(conv_lines(terms, base, lines, weight_one), 0.0).astype(BF16)
        terms = [(field, 0, tap(1, odd)), (field, 1, tap(2, odd))]
        part_two[spot] = conv_lines(terms, base, lines, weight_one)
        part_one[spot] = conv_lines([(field, 0, tap(2, odd))], base, lines, weight_one)


def kernel_a1(*refs, chans, sides):
    own, own_halos = refs[0], refs[1 : 1 + sides]
    near, near_halos = refs[1 + sides], refs[2 + sides : 2 + 2 * sides]
    done_three, done_four, weight_one, weight_two = refs[2 + 2 * sides : 6 + 2 * sides]
    out_two, out_three = refs[6 + 2 * sides : 8 + 2 * sides]
    parts = refs[8 + 2 * sides : 8 + 4 * sides]
    field, layer = refs[8 + 4 * sides :]
    odd = lax.rem(lax.axis_index("brick"), 2)
    size_y = own.shape[1]
    first, rows = inner_rows(chans, size_y)
    layer[0, pl.ds(first + 1, rows)] = done_three[...]
    layer[1, pl.ds(first + 1, rows)] = done_four[...]
    for side, (start, count) in enumerate(border_rows(chans, size_y)):
        pairs = ((own, own_halos[side], odd), (own, own_halos[side], 1 - odd))
        pairs += ((near, near_halos[side], odd), (near, near_halos[side], 1 - odd))
        fill_border(field, start, size_y, [(block, plane, halo, plane) for block, halo, plane in pairs])
        for slot in range(2):
            terms = [(field, slot + step, tap(step, odd)) for step in range(3)]
            value = jnp.maximum(conv_lines(terms, 0, count, weight_one), 0.0).astype(BF16)
            layer[slot, pl.ds(start + 1, count)] = value
        terms = [(field, 0, tap(1, odd)), (field, 1, tap(2, odd))]
        parts[sides + side][...] = conv_lines(terms, 0, count, weight_one)
        parts[side][...] = conv_lines([(field, 0, tap(2, odd))], 0, count, weight_one)
    for slot in range(2):
        clear_outside(layer, slot, chans)
    lines = tile_of(size_y)
    for row in range(0, size_y, lines):
        spot = pl.ds(row, lines)
        out_two[spot] = conv_lines([(layer, 0, tap(2, odd))], row, lines, weight_two)
        out_three[spot] = conv_lines([(layer, 0, tap(1, odd)), (layer, 1, tap(2, odd))], row, lines, weight_two)


def kernel_b0(plane_one, plane_zero, part_one, part_two, weight_one, done_one, done_two, field, *, chans):
    odd = lax.rem(lax.axis_index("brick"), 2)
    valid = has_far()
    fill_inner(field, ((plane_zero, None), (plane_one, None)), valid)
    first, rows = inner_rows(chans, plane_one.shape[0])
    lines = tile_of(rows)
    for row in range(0, rows, lines):
        spot, base = pl.ds(row, lines), first + row
        value = conv_lines([(field, 0, tap(0, odd)), (field, 1, tap(1, odd))], base, lines, weight_one)
        value = jnp.maximum(value + part_one[spot], 0.0)
        done_one[spot] = jnp.where(valid, value, 0.0).astype(BF16)
        value = conv_lines([(field, 1, tap(0, odd))], base, lines, weight_one)
        done_two[spot] = jnp.maximum(value + part_two[spot], 0.0).astype(BF16)


def kernel_b1(*refs, chans, sides):
    plane_one, plane_zero, halos = refs[0], refs[1], refs[2 : 2 + sides]
    done_one, done_two, out_two, out_three, weight_one, weight_two = refs[2 + sides : 8 + sides]
    parts = refs[8 + sides : 8 + 3 * sides]
    skipped_two, skipped_three, pooled, field, layer, sums = refs[8 + 3 * sides :]
    odd = lax.rem(lax.axis_index("brick"), 2)
    valid = has_far()
    size_y, depth = plane_one.shape[0], plane_one.shape[1]
    first, rows = inner_rows(chans, size_y)
    layer[0, pl.ds(first + 1, rows)] = done_one[...]
    layer[1, pl.ds(first + 1, rows)] = done_two[...]
    for side, (start, count) in enumerate(border_rows(chans, size_y)):
        planes = ((plane_zero, None, halos[side], odd), (plane_one, None, halos[side], 1 - odd))
        fill_border(field, start, size_y, planes, valid)
        value = conv_lines([(field, 0, tap(0, odd)), (field, 1, tap(1, odd))], 0, count, weight_one)
        value = jnp.maximum(value + parts[side][...], 0.0)
        layer[0, pl.ds(start + 1, count)] = jnp.where(valid, value, 0.0).astype(BF16)
        value = conv_lines([(field, 1, tap(0, odd))], 0, count, weight_one)
        layer[1, pl.ds(start + 1, count)] = jnp.maximum(value + parts[sides + side][...], 0.0).astype(BF16)
    for slot in range(2):
        clear_outside(layer, slot, chans)
    lines = tile_of(size_y)
    for row in range(0, size_y, lines):
        spot = pl.ds(row, lines)
        value = conv_lines([(layer, 0, tap(0, odd)), (layer, 1, tap(1, odd))], row, lines, weight_two)
        two = jnp.maximum(value + out_two[spot], 0.0).astype(BF16)
        skipped_two[spot] = two
        value = conv_lines([(layer, 1, tap(0, odd))], row, lines, weight_two)
        three = jnp.maximum(value + out_three[spot], 0.0).astype(BF16)
        skipped_three[spot] = three
        both = two.astype(F32) + three.astype(F32)
        for group in range(sums.shape[0]):
            sums[group, spot] = both[:, :, group * LANES : (group + 1) * LANES]
    for row in range(size_y // 2):
        for group in range(sums.shape[0]):
            pairs = [
                sums[group, 2 * row + step, pl.ds(side, depth // 2, stride=2)] for step in range(2) for side in range(2)
            ]
            mean = (pairs[0] + pairs[1] + pairs[2] + pairs[3]) * 0.125
            pooled[row, :, group * LANES : (group + 1) * LANES] = mean.astype(BF16)


def fill_pooled(target, planes, valid=None):
    chan, chans = lax.axis_index("chan"), len(planes[0])
    zeros = jnp.zeros(target.shape[2:], target.dtype)
    for slot, blocks in enumerate(planes):
        rows = blocks[0].shape[0]
        target[slot, 0] = zeros
        target[slot, chans * rows + 1] = zeros
        for step, block in enumerate(blocks):
            source = lax.rem(chan - step + chans, chans)
            value = block[...]
            if valid is not None:
                value = jnp.where(valid, value, jnp.zeros_like(value))
            target[slot, pl.ds(1 + source * rows, rows)] = value


def kernel_c1(*refs, chans):
    weight, part, field = refs[2 * chans :]
    odd = lax.rem(lax.axis_index("brick"), 2)
    fill_pooled(field, (refs[:chans], refs[chans : 2 * chans]))
    lines = tile_of(part.shape[0])
    for row in range(0, part.shape[0], lines):
        part[pl.ds(row, lines)] = conv_lines([(field, 0, tap(1, odd)), (field, 1, tap(2, odd))], row, lines, weight)


def kernel_c2(*refs, chans):
    part, weight, projection, own_part = refs[chans : chans + 4]
    sent = refs[chans + 4 : 2 * chans + 3]
    field, parts = refs[2 * chans + 3 :]
    odd = lax.rem(lax.axis_index("brick"), 2)
    chan = lax.axis_index("chan")
    total, depth = part.shape[0], part.shape[1]
    rows = total // chans
    fill_pooled(field, (refs[:chans],), has_far())
    lines = tile_of(total)
    for row in range(0, total, lines):
        value = conv_lines([(field, 0, tap(0, odd))], row, lines, weight) + part[pl.ds(row, lines)]
        value = jnp.maximum(value, 0.0).astype(BF16).reshape(lines * depth, weight.shape[4])
        lifted = jnp.dot(value, projection[...], preferred_element_type=F32)
        parts[pl.ds(row, lines)] = lifted.reshape(lines, depth, lifted.shape[1])
    own_part[...] = parts[pl.ds(chan * rows, rows)]
    for step in range(1, chans):
        target = lax.rem(chan + step, chans)
        sent[step - 1][...] = parts[pl.ds(target * rows, rows)].astype(BF16)


def kernel_d(*refs):
    skipped_two, skipped_three, own_part = refs[:3]
    received, merged, fine = refs[3:-2], refs[-2], refs[-1]
    odd = lax.rem(lax.axis_index("brick"), 2)
    rows, depth = own_part.shape[0], own_part.shape[1]
    lifted = own_part[...]
    for part in received:
        lifted = lifted + part[...].astype(F32)
    for group in range(fine.shape[0]):
        lanes = slice(group * LANES, (group + 1) * LANES)
        for row in range(rows):
            for side in range(2):
                fine[group, row, pl.ds(side, depth, stride=2)] = lifted[row, :, lanes]
        for row in range(rows):
            value = fine[group, row]
            for plane, skipped in ((odd, skipped_two), (1 - odd, skipped_three)):
                for step in range(2):
                    line = 2 * row + step
                    merged[plane, line, :, lanes] = (skipped[line, :, lanes].astype(F32) + value).astype(BF16)


def shards(volume, first_weight, second_weight, coarse_weight, projection):
    chans = lax.axis_size("chan")
    size_x, size_y, depth, channels = volume.shape
    assert size_x == 2 and lax.axis_size("brick") % 2 == 0

    turns = [[], [lambda c: 1 - c]][chans - 1] if chans <= 2 else [lambda c: c + 1, lambda c: c - 1]
    near = exchange(volume, "near")
    token = call(early, [], [((8, LANES), F32)], [], WEIGHT_COPY_FLOPS, 4)[0]
    plane_shape, sides = (size_y, depth, channels), len(turns)
    first, second, *edges = call(
        functools.partial(pieces_to_send, chans=chans),
        [volume, token],
        [(plane_shape, BF16)] * 2 + [((2, 2, depth, channels), BF16)] * sides,
        [],
        WEIGHT_COPY_FLOPS,
        4,
    )
    own_halos = [exchange(edge, "own", turn) for edge, turn in zip(edges, turns)]
    far_one = exchange(first, "far")
    far_halos = [exchange(halo, "far") for halo in own_halos]
    far_zero = exchange(second, "far")
    near_halos = [exchange(halo, "near") for halo in own_halos]

    static = dict(chans=chans, sides=sides)
    inner = inner_rows(chans, size_y)[1]
    border_shape = (2, depth, channels)
    line_flops = 2 * depth * 9 * channels * channels
    done_three, done_four, part_one, part_two = call(
        functools.partial(kernel_a0, chans=chans),
        [volume, near, first_weight],
        [((inner, depth, channels), BF16)] * 2 + [((inner, depth, channels), F32)] * 2,
        [pltpu.VMEM((4, size_y + 2, depth, channels), BF16)],
        9 * inner * line_flops,
        12,
    )
    out_two, out_three, *border = call(
        functools.partial(kernel_a1, **static),
        [volume, *own_halos, near, *near_halos, done_three, done_four, first_weight, second_weight],
        [(plane_shape, F32)] * 2 + [(border_shape, F32)] * (2 * sides),
        [pltpu.VMEM((4, 4, depth, channels), BF16), pltpu.VMEM((2, size_y + 2, depth, channels), BF16)],
        (18 * sides + 3 * size_y) * line_flops,
        12,
    )
    done_one, done_two = call(
        functools.partial(kernel_b0, chans=chans),
        [far_one, far_zero, part_one, part_two, first_weight],
        [((inner, depth, channels), BF16)] * 2,
        [pltpu.VMEM((2, size_y + 2, depth, channels), BF16)],
        3 * inner * line_flops,
        12,
    )
    skipped_two, skipped_three, pooled = call(
        functools.partial(kernel_b1, **static),
        [far_one, far_zero, *far_halos, done_one, done_two, out_two, out_three, first_weight, second_weight, *border],
        [(plane_shape, BF16)] * 2 + [((size_y // 2, depth // 2, channels), BF16)],
        [
            pltpu.VMEM((2, 4, depth, channels), BF16),
            pltpu.VMEM((2, size_y + 2, depth, channels), BF16),
            pltpu.VMEM((channels // LANES, size_y, depth, LANES), F32),
        ],
        (6 * sides + 3 * size_y) * line_flops,
        12,
    )

    turns = [(lambda c, step=step: (c + step) % chans) for step in range(chans)]
    own_blocks = [pooled] + [exchange(pooled, "own", turn) for turn in turns[1:]]
    far_blocks = [exchange(pooled, "far", turn) for turn in turns[1:]]
    far_blocks = [exchange(pooled, "far")] + far_blocks
    near_blocks = [exchange(pooled, "near")]
    near_blocks += [exchange(block, "near") for block in own_blocks[1:]]
    part_shape = (size_y // 2, depth // 2, channels)
    coarse_rows = chans * size_y // 2
    coarse_channels = coarse_weight.shape[4]
    plane_flops = 2 * coarse_rows * (depth // 2) * 9 * channels * coarse_channels
    coarse_field = (coarse_rows + 2, depth // 2, channels)
    coarse_part = call(
        functools.partial(kernel_c1, chans=chans),
        [*own_blocks, *near_blocks, coarse_weight],
        [((coarse_rows, depth // 2, coarse_channels), F32)],
        [pltpu.VMEM((2,) + coarse_field, BF16)],
        2 * plane_flops,
        12,
    )[0]
    parts = call(
        functools.partial(kernel_c2, chans=chans),
        [*far_blocks, coarse_part, coarse_weight, projection],
        [(part_shape, F32)] + [(part_shape, BF16)] * (chans - 1),
        [pltpu.VMEM((1,) + coarse_field, BF16), pltpu.VMEM((coarse_rows, depth // 2, channels), F32)],
        plane_flops,
        12,
    )
    received = [exchange(part, "own", turn) for part, turn in zip(parts[1:], turns[1:])]
    return call(
        kernel_d,
        [skipped_two, skipped_three, parts[0], *received],
        [(volume.shape, BF16)],
        [pltpu.VMEM((channels // LANES, size_y // 2, depth, LANES), F32)],
        volume.size,
        16,
        results_in_vmem=False,
    )[0]


def solution(mesh):
    in_specs = (
        P("brick", "chan", None, None),
        P(),
        P(),
        P(None, None, None, None, "chan"),
        P("chan", None),
    )
    out_specs = P("brick", "chan", None, None)

    return jax.shard_map(shards, mesh=mesh, in_specs=in_specs, out_specs=out_specs, check_vma=False)
```

```python
import functools

import jax
import jax.numpy as jnp
from jax import lax
from jax.experimental import pallas as pl
from jax.experimental.pallas import tpu as pltpu
from jax.sharding import PartitionSpec as P


AXES = ("brick", "chan")
BF16 = jnp.bfloat16
F32 = jnp.float32
LANES = 128
WEIGHT_COPY_FLOPS = 2**33
VMEM_SPEC = pl.BlockSpec(memory_space=pltpu.VMEM)


def brick_partner(kind, brick, bricks):
    if kind == "own":
        return brick
    partner = brick ^ 1 if kind == "near" else ((brick + 1) ^ 1) - 1
    return partner if 0 <= partner < bricks else None


def exchange(value, kind, chan_of=None):
    bricks, chans = lax.axis_size("brick"), lax.axis_size("chan")
    pairs = []
    for brick in range(bricks):
        for chan in range(chans):
            other = brick_partner(kind, brick, bricks)
            target = chan if chan_of is None else chan_of(chan)
            if other is None and chans % 2 == 0:
                other, target = brick, chan ^ 1
            if other is not None and 0 <= target < chans:
                pairs.append((brick * chans + chan, other * chans + target))
    return lax.ppermute(value, AXES, pairs)


def has_far():
    brick = lax.axis_index("brick")
    edge = brick + lax.rem(brick, 2)
    return jnp.logical_and(edge > 0, edge < lax.axis_size("brick"))


def early(out):
    out[...] = jnp.zeros_like(out)


def pieces_to_send(volume, _, first, second, *edges, chans):
    odd = lax.rem(lax.axis_index("brick"), 2)
    size_y = volume.shape[1]
    first[...] = volume[odd]
    second[...] = volume[1 - odd]
    starts = [jnp.where(lax.axis_index("chan") == 0, size_y - 2, 0)] if chans == 2 else [size_y - 2, 0]
    for edge, start in zip(edges, starts):
        edge[...] = volume[:, pl.ds(start, 2)]


def call(kernel, inputs, outputs, scratch, flops, limit_mib, results_in_vmem=True):
    inputs = [pltpu.with_memory_space_constraint(value, pltpu.VMEM) for value in inputs]
    if results_in_vmem:
        out_shape = [pltpu.VMEM(shape, dtype) for shape, dtype in outputs]
    else:
        out_shape = [jax.ShapeDtypeStruct(shape, dtype) for shape, dtype in outputs]
    return pl.pallas_call(
        kernel,
        out_shape=out_shape,
        in_specs=[VMEM_SPEC] * len(inputs),
        out_specs=[VMEM_SPEC] * len(outputs),
        scratch_shapes=scratch,
        compiler_params=pltpu.CompilerParams(vmem_limit_bytes=limit_mib * 2**20),
        cost_estimate=pl.CostEstimate(flops=flops, bytes_accessed=2**20, transcendentals=0),
    )(*inputs)


def tile_of(rows):
    return max(lines for lines in range(1, 10) if rows % lines == 0)


def conv_lines(terms, row, lines, weight):
    sums = []
    for dz in range(3):
        total = None
        for ref, plane, dx in terms:
            for dy in range(3):
                window = ref[plane, pl.ds(row + dy, lines)]
                window = window.reshape(lines * window.shape[1], window.shape[2])
                part = jnp.dot(window, weight[dx, dy, dz], preferred_element_type=F32)
                total = part if total is None else total + part
        sums.append(total)
    depth = terms[0][0].shape[2]
    count = sums[0].shape[0]
    place = lax.rem(lax.broadcasted_iota(jnp.int32, sums[0].shape, 0), depth)
    before = jnp.where(place == 0, 0.0, pltpu.roll(sums[0], 1, 0))
    after = jnp.where(place == depth - 1, 0.0, pltpu.roll(sums[2], count - 1, 0))
    return (before + sums[1] + after).reshape(lines, depth, sums[0].shape[1])


def tap(step, odd):
    return step + odd * (2 - 2 * step)


def inner_rows(chans, size_y):
    return {1: (0, size_y), 2: (lax.axis_index("chan"), size_y - 1)}.get(chans, (1, size_y - 2))


def border_rows(chans, size_y):
    if chans == 1:
        return []
    if chans == 2:
        return [(jnp.where(lax.axis_index("chan") == 0, size_y - 1, -1), 2)]
    return [(-1, 2), (size_y - 1, 2)]


def fill_inner(target, planes, valid=None):
    size_y = target.shape[1] - 2
    zeros = jnp.zeros(target.shape[2:], target.dtype)
    for slot, (block, plane) in enumerate(planes):
        rows = block[...] if plane is None else block[plane]
        target[slot, 0] = zeros
        target[slot, 1 : size_y + 1] = rows if valid is None else jnp.where(valid, rows, jnp.zeros_like(rows))
        target[slot, size_y + 1] = zeros


def fill_border(target, start, size_y, planes, valid=None):
    high = start > 0
    place, source = jnp.where(high, 0, 2), jnp.where(high, size_y - 2, 0)
    for slot, (block, plane, halo, halo_plane) in enumerate(planes):
        rows = block[pl.ds(source, 2)] if plane is None else block[plane, pl.ds(source, 2)]
        beyond = halo[halo_plane]
        if valid is not None:
            rows = jnp.where(valid, rows, jnp.zeros_like(rows))
            beyond = jnp.where(valid, beyond, jnp.zeros_like(beyond))
        target[slot, pl.ds(place, 2)] = rows
        target[slot, pl.ds(2 - place, 2)] = beyond


def clear_outside(layer, slot, chans):
    chan = lax.axis_index("chan")
    last = layer.shape[1] - 1
    for row, owner in ((0, 0), (last, chans - 1)):
        if chans <= 2:
            keep = jnp.logical_and(chans == 2, chan != owner)
        else:
            keep = chan != owner
        layer[slot, row] = jnp.where(keep, layer[slot, row], jnp.zeros_like(layer[slot, row]))


def kernel_a0(own, near, weight_one, done_three, done_four, part_one, part_two, field, *, chans):
    odd = lax.rem(lax.axis_index("brick"), 2)
    size_y = own.shape[1]
    fill_inner(field, ((own, odd), (own, 1 - odd), (near, odd), (near, 1 - odd)))
    first, rows = inner_rows(chans, size_y)
    lines = tile_of(rows)
    for row in range(0, rows, lines):
        spot, base = pl.ds(row, lines), first + row
        for slot, done in enumerate((done_three, done_four)):
            terms = [(field, slot + step, tap(step, odd)) for step in range(3)]
            done[spot] = jnp.maximum(conv_lines(terms, base, lines, weight_one), 0.0).astype(BF16)
        terms = [(field, 0, tap(1, odd)), (field, 1, tap(2, odd))]
        part_two[spot] = conv_lines(terms, base, lines, weight_one)
        part_one[spot] = conv_lines([(field, 0, tap(2, odd))], base, lines, weight_one)


def kernel_a1(*refs, chans, sides):
    own, own_halos = refs[0], refs[1 : 1 + sides]
    near, near_halos = refs[1 + sides], refs[2 + sides : 2 + 2 * sides]
    done_three, done_four, weight_one, weight_two = refs[2 + 2 * sides : 6 + 2 * sides]
    out_two, out_three = refs[6 + 2 * sides : 8 + 2 * sides]
    parts = refs[8 + 2 * sides : 8 + 4 * sides]
    field, layer = refs[8 + 4 * sides :]
    odd = lax.rem(lax.axis_index("brick"), 2)
    size_y = own.shape[1]
    first, rows = inner_rows(chans, size_y)
    layer[0, pl.ds(first + 1, rows)] = done_three[...]
    layer[1, pl.ds(first + 1, rows)] = done_four[...]
    for side, (start, count) in enumerate(border_rows(chans, size_y)):
        pairs = ((own, own_halos[side], odd), (own, own_halos[side], 1 - odd))
        pairs += ((near, near_halos[side], odd), (near, near_halos[side], 1 - odd))
        fill_border(field, start, size_y, [(block, plane, halo, plane) for block, halo, plane in pairs])
        for slot in range(2):
            terms = [(field, slot + step, tap(step, odd)) for step in range(3)]
            value = jnp.maximum(conv_lines(terms, 0, count, weight_one), 0.0).astype(BF16)
            layer[slot, pl.ds(start + 1, count)] = value
        terms = [(field, 0, tap(1, odd)), (field, 1, tap(2, odd))]
        parts[sides + side][...] = conv_lines(terms, 0, count, weight_one)
        parts[side][...] = conv_lines([(field, 0, tap(2, odd))], 0, count, weight_one)
    for slot in range(2):
        clear_outside(layer, slot, chans)
    lines = tile_of(size_y)
    for row in range(0, size_y, lines):
        spot = pl.ds(row, lines)
        out_two[spot] = conv_lines([(layer, 0, tap(2, odd))], row, lines, weight_two)
        out_three[spot] = conv_lines([(layer, 0, tap(1, odd)), (layer, 1, tap(2, odd))], row, lines, weight_two)


def kernel_m(plane_one, part_one, part_two, weight_one, more_one, done_two, field, *, chans):
    odd = lax.rem(lax.axis_index("brick"), 2)
    fill_inner(field, ((plane_one, None),), has_far())
    first, rows = inner_rows(chans, plane_one.shape[0])
    lines = tile_of(rows)
    for row in range(0, rows, lines):
        spot, base = pl.ds(row, lines), first + row
        value = conv_lines([(field, 0, tap(0, odd))], base, lines, weight_one)
        done_two[spot] = jnp.maximum(value + part_two[spot], 0.0).astype(BF16)
        more_one[spot] = part_one[spot] + conv_lines([(field, 0, tap(1, odd))], base, lines, weight_one)


def kernel_b0(plane_zero, part_one, weight_one, done_one, field, *, chans):
    odd = lax.rem(lax.axis_index("brick"), 2)
    valid = has_far()
    fill_inner(field, ((plane_zero, None),), valid)
    first, rows = inner_rows(chans, plane_zero.shape[0])
    lines = tile_of(rows)
    for row in range(0, rows, lines):
        spot = pl.ds(row, lines)
        value = conv_lines([(field, 0, tap(0, odd))], first + row, lines, weight_one)
        done_one[spot] = jnp.where(valid, jnp.maximum(value + part_one[spot], 0.0), 0.0).astype(BF16)


def kernel_b1(*refs, chans, sides):
    plane_one, plane_zero, halos = refs[0], refs[1], refs[2 : 2 + sides]
    done_one, done_two, out_two, out_three, weight_one, weight_two = refs[2 + sides : 8 + sides]
    parts = refs[8 + sides : 8 + 3 * sides]
    skipped_two, skipped_three, pooled, field, layer, sums = refs[8 + 3 * sides :]
    odd = lax.rem(lax.axis_index("brick"), 2)
    valid = has_far()
    size_y, depth = plane_one.shape[0], plane_one.shape[1]
    first, rows = inner_rows(chans, size_y)
    layer[0, pl.ds(first + 1, rows)] = done_one[...]
    layer[1, pl.ds(first + 1, rows)] = done_two[...]
    for side, (start, count) in enumerate(border_rows(chans, size_y)):
        planes = ((plane_zero, None, halos[side], odd), (plane_one, None, halos[side], 1 - odd))
        fill_border(field, start, size_y, planes, valid)
        value = conv_lines([(field, 0, tap(0, odd)), (field, 1, tap(1, odd))], 0, count, weight_one)
        value = jnp.maximum(value + parts[side][...], 0.0)
        layer[0, pl.ds(start + 1, count)] = jnp.where(valid, value, 0.0).astype(BF16)
        value = conv_lines([(field, 1, tap(0, odd))], 0, count, weight_one)
        layer[1, pl.ds(start + 1, count)] = jnp.maximum(value + parts[sides + side][...], 0.0).astype(BF16)
    for slot in range(2):
        clear_outside(layer, slot, chans)
    lines = tile_of(size_y)
    for row in range(0, size_y, lines):
        spot = pl.ds(row, lines)
        value = conv_lines([(layer, 0, tap(0, odd)), (layer, 1, tap(1, odd))], row, lines, weight_two)
        two = jnp.maximum(value + out_two[spot], 0.0).astype(BF16)
        skipped_two[spot] = two
        value = conv_lines([(layer, 1, tap(0, odd))], row, lines, weight_two)
        three = jnp.maximum(value + out_three[spot], 0.0).astype(BF16)
        skipped_three[spot] = three
        both = two.astype(F32) + three.astype(F32)
        for group in range(sums.shape[0]):
            sums[group, spot] = both[:, :, group * LANES : (group + 1) * LANES]
    for row in range(size_y // 2):
        for group in range(sums.shape[0]):
            pairs = [
                sums[group, 2 * row + step, pl.ds(side, depth // 2, stride=2)] for step in range(2) for side in range(2)
            ]
            mean = (pairs[0] + pairs[1] + pairs[2] + pairs[3]) * 0.125
            pooled[row, :, group * LANES : (group + 1) * LANES] = mean.astype(BF16)


def fill_pooled(target, planes, valid=None):
    chan, chans = lax.axis_index("chan"), len(planes[0])
    zeros = jnp.zeros(target.shape[2:], target.dtype)
    for slot, blocks in enumerate(planes):
        rows = blocks[0].shape[0]
        target[slot, 0] = zeros
        target[slot, chans * rows + 1] = zeros
        for step, block in enumerate(blocks):
            source = lax.rem(chan - step + chans, chans)
            value = block[...]
            if valid is not None:
                value = jnp.where(valid, value, jnp.zeros_like(value))
            target[slot, pl.ds(1 + source * rows, rows)] = value


def kernel_c1(*refs, chans):
    weight, part, field = refs[2 * chans :]
    odd = lax.rem(lax.axis_index("brick"), 2)
    fill_pooled(field, (refs[:chans], refs[chans : 2 * chans]))
    lines = tile_of(part.shape[0])
    for row in range(0, part.shape[0], lines):
        part[pl.ds(row, lines)] = conv_lines([(field, 0, tap(1, odd)), (field, 1, tap(2, odd))], row, lines, weight)


def kernel_c2(*refs, chans):
    part, weight, projection, own_part = refs[chans : chans + 4]
    sent = refs[chans + 4 : 2 * chans + 3]
    field, parts = refs[2 * chans + 3 :]
    odd = lax.rem(lax.axis_index("brick"), 2)
    chan = lax.axis_index("chan")
    total, depth = part.shape[0], part.shape[1]
    rows = total // chans
    fill_pooled(field, (refs[:chans],), has_far())
    lines = tile_of(total)
    for row in range(0, total, lines):
        value = conv_lines([(field, 0, tap(0, odd))], row, lines, weight) + part[pl.ds(row, lines)]
        value = jnp.maximum(value, 0.0).astype(BF16).reshape(lines * depth, weight.shape[4])
        lifted = jnp.dot(value, projection[...], preferred_element_type=F32)
        parts[pl.ds(row, lines)] = lifted.reshape(lines, depth, lifted.shape[1])
    own_part[...] = parts[pl.ds(chan * rows, rows)]
    for step in range(1, chans):
        target = lax.rem(chan + step, chans)
        sent[step - 1][...] = parts[pl.ds(target * rows, rows)].astype(BF16)


def kernel_d(*refs):
    skipped_two, skipped_three, own_part = refs[:3]
    received, merged, fine = refs[3:-2], refs[-2], refs[-1]
    odd = lax.rem(lax.axis_index("brick"), 2)
    rows, depth = own_part.shape[0], own_part.shape[1]
    lifted = own_part[...]
    for part in received:
        lifted = lifted + part[...].astype(F32)
    for group in range(fine.shape[0]):
        lanes = slice(group * LANES, (group + 1) * LANES)
        for row in range(rows):
            for side in range(2):
                fine[group, row, pl.ds(side, depth, stride=2)] = lifted[row, :, lanes]
        for row in range(rows):
            value = fine[group, row]
            for plane, skipped in ((odd, skipped_two), (1 - odd, skipped_three)):
                for step in range(2):
                    line = 2 * row + step
                    merged[plane, line, :, lanes] = (skipped[line, :, lanes].astype(F32) + value).astype(BF16)


def shards(volume, first_weight, second_weight, coarse_weight, projection):
    chans = lax.axis_size("chan")
    size_x, size_y, depth, channels = volume.shape
    assert size_x == 2 and lax.axis_size("brick") % 2 == 0

    turns = [[], [lambda c: 1 - c]][chans - 1] if chans <= 2 else [lambda c: c + 1, lambda c: c - 1]
    near = exchange(volume, "near")
    token = call(early, [], [((8, LANES), F32)], [], WEIGHT_COPY_FLOPS, 4)[0]
    plane_shape, sides = (size_y, depth, channels), len(turns)
    first, second, *edges = call(
        functools.partial(pieces_to_send, chans=chans),
        [volume, token],
        [(plane_shape, BF16)] * 2 + [((2, 2, depth, channels), BF16)] * sides,
        [],
        WEIGHT_COPY_FLOPS,
        4,
    )
    own_halos = [exchange(edge, "own", turn) for edge, turn in zip(edges, turns)]
    far_one = exchange(first, "far")
    far_halos = [exchange(halo, "far") for halo in own_halos]
    far_zero = exchange(second, "far")
    near_halos = [exchange(halo, "near") for halo in own_halos]

    static = dict(chans=chans, sides=sides)
    inner = inner_rows(chans, size_y)[1]
    border_shape = (2, depth, channels)
    line_flops = 2 * depth * 9 * channels * channels
    done_three, done_four, part_one, part_two = call(
        functools.partial(kernel_a0, chans=chans),
        [volume, near, first_weight],
        [((inner, depth, channels), BF16)] * 2 + [((inner, depth, channels), F32)] * 2,
        [pltpu.VMEM((4, size_y + 2, depth, channels), BF16)],
        9 * inner * line_flops,
        12,
    )
    part_one, done_two = call(
        functools.partial(kernel_m, chans=chans),
        [far_one, part_one, part_two, first_weight],
        [((inner, depth, channels), F32), ((inner, depth, channels), BF16)],
        [pltpu.VMEM((1, size_y + 2, depth, channels), BF16)],
        2 * inner * line_flops,
        12,
    )
    out_two, out_three, *border = call(
        functools.partial(kernel_a1, **static),
        [volume, *own_halos, near, *near_halos, done_three, done_four, first_weight, second_weight],
        [(plane_shape, F32)] * 2 + [(border_shape, F32)] * (2 * sides),
        [pltpu.VMEM((4, 4, depth, channels), BF16), pltpu.VMEM((2, size_y + 2, depth, channels), BF16)],
        (18 * sides + 3 * size_y) * line_flops,
        12,
    )
    done_one = call(
        functools.partial(kernel_b0, chans=chans),
        [far_zero, part_one, first_weight],
        [((inner, depth, channels), BF16)],
        [pltpu.VMEM((1, size_y + 2, depth, channels), BF16)],
        inner * line_flops,
        12,
    )[0]
    skipped_two, skipped_three, pooled = call(
        functools.partial(kernel_b1, **static),
        [far_one, far_zero, *far_halos, done_one, done_two, out_two, out_three, first_weight, second_weight, *border],
        [(plane_shape, BF16)] * 2 + [((size_y // 2, depth // 2, channels), BF16)],
        [
            pltpu.VMEM((2, 4, depth, channels), BF16),
            pltpu.VMEM((2, size_y + 2, depth, channels), BF16),
            pltpu.VMEM((channels // LANES, size_y, depth, LANES), F32),
        ],
        (6 * sides + 3 * size_y) * line_flops,
        12,
    )

    turns = [(lambda c, step=step: (c + step) % chans) for step in range(chans)]
    own_blocks = [pooled] + [exchange(pooled, "own", turn) for turn in turns[1:]]
    far_blocks = [exchange(pooled, "far", turn) for turn in turns[1:]]
    far_blocks = [exchange(pooled, "far")] + far_blocks
    near_blocks = [exchange(pooled, "near")]
    near_blocks += [exchange(block, "near") for block in own_blocks[1:]]
    part_shape = (size_y // 2, depth // 2, channels)
    coarse_rows = chans * size_y // 2
    coarse_channels = coarse_weight.shape[4]
    plane_flops = 2 * coarse_rows * (depth // 2) * 9 * channels * coarse_channels
    coarse_field = (coarse_rows + 2, depth // 2, channels)
    coarse_part = call(
        functools.partial(kernel_c1, chans=chans),
        [*own_blocks, *near_blocks, coarse_weight],
        [((coarse_rows, depth // 2, coarse_channels), F32)],
        [pltpu.VMEM((2,) + coarse_field, BF16)],
        2 * plane_flops,
        12,
    )[0]
    parts = call(
        functools.partial(kernel_c2, chans=chans),
        [*far_blocks, coarse_part, coarse_weight, projection],
        [(part_shape, F32)] + [(part_shape, BF16)] * (chans - 1),
        [pltpu.VMEM((1,) + coarse_field, BF16), pltpu.VMEM((coarse_rows, depth // 2, channels), F32)],
        plane_flops,
        12,
    )
    received = [exchange(part, "own", turn) for part, turn in zip(parts[1:], turns[1:])]
    return call(
        kernel_d,
        [skipped_two, skipped_three, parts[0], *received],
        [(volume.shape, BF16)],
        [pltpu.VMEM((channels // LANES, size_y // 2, depth, LANES), F32)],
        volume.size,
        16,
        results_in_vmem=False,
    )[0]


def solution(mesh):
    in_specs = (
        P("brick", "chan", None, None),
        P(),
        P(),
        P(None, None, None, None, "chan"),
        P("chan", None),
    )
    out_specs = P("brick", "chan", None, None)

    return jax.shard_map(shards, mesh=mesh, in_specs=in_specs, out_specs=out_specs, check_vma=False)
```

```python
import functools

import jax
import jax.numpy as jnp
from jax import lax
from jax.experimental import pallas as pl
from jax.experimental.pallas import tpu as pltpu
from jax.sharding import PartitionSpec as P


AXES = ("brick", "chan")
BF16 = jnp.bfloat16
F32 = jnp.float32
LANES = 128
WEIGHT_COPY_FLOPS = 2**33
VMEM_SPEC = pl.BlockSpec(memory_space=pltpu.VMEM)


def brick_partner(kind, brick, bricks):
    if kind == "own":
        return brick
    partner = brick ^ 1 if kind == "near" else ((brick + 1) ^ 1) - 1
    return partner if 0 <= partner < bricks else None


def exchange(value, kind, chan_of=None):
    bricks, chans = lax.axis_size("brick"), lax.axis_size("chan")
    pairs = []
    for brick in range(bricks):
        for chan in range(chans):
            other = brick_partner(kind, brick, bricks)
            target = chan if chan_of is None else chan_of(chan)
            if other is None and chans % 2 == 0:
                other, target = brick, chan ^ 1
            if other is not None and 0 <= target < chans:
                pairs.append((brick * chans + chan, other * chans + target))
    return lax.ppermute(value, AXES, pairs)


def has_far():
    brick = lax.axis_index("brick")
    edge = brick + lax.rem(brick, 2)
    return jnp.logical_and(edge > 0, edge < lax.axis_size("brick"))


def early(out):
    out[...] = jnp.zeros_like(out)


def pieces_to_send(volume, _, first, second, *edges, chans):
    odd = lax.rem(lax.axis_index("brick"), 2)
    size_y = volume.shape[1]
    first[...] = volume[odd]
    second[...] = volume[1 - odd]
    starts = [jnp.where(lax.axis_index("chan") == 0, size_y - 2, 0)] if chans == 2 else [size_y - 2, 0]
    for edge, start in zip(edges, starts):
        edge[...] = volume[:, pl.ds(start, 2)]


def call(kernel, inputs, outputs, scratch, flops, limit_mib, results_in_vmem=True):
    inputs = [pltpu.with_memory_space_constraint(value, pltpu.VMEM) for value in inputs]
    if results_in_vmem:
        out_shape = [pltpu.VMEM(shape, dtype) for shape, dtype in outputs]
    else:
        out_shape = [jax.ShapeDtypeStruct(shape, dtype) for shape, dtype in outputs]
    return pl.pallas_call(
        kernel,
        out_shape=out_shape,
        in_specs=[VMEM_SPEC] * len(inputs),
        out_specs=[VMEM_SPEC] * len(outputs),
        scratch_shapes=scratch,
        compiler_params=pltpu.CompilerParams(vmem_limit_bytes=limit_mib * 2**20),
        cost_estimate=pl.CostEstimate(flops=flops, bytes_accessed=2**20, transcendentals=0),
    )(*inputs)


def tile_of(rows):
    return max(lines for lines in range(1, 10) if rows % lines == 0)


def conv_lines(terms, row, lines, weight):
    sums = []
    for dz in range(3):
        total = None
        for ref, plane, dx in terms:
            for dy in range(3):
                window = ref[plane, pl.ds(row + dy, lines)]
                window = window.reshape(lines * window.shape[1], window.shape[2])
                part = jnp.dot(window, weight[dx, dy, dz], preferred_element_type=F32)
                total = part if total is None else total + part
        sums.append(total)
    depth = terms[0][0].shape[2]
    count = sums[0].shape[0]
    place = lax.rem(lax.broadcasted_iota(jnp.int32, sums[0].shape, 0), depth)
    before = jnp.where(place == 0, 0.0, pltpu.roll(sums[0], 1, 0))
    after = jnp.where(place == depth - 1, 0.0, pltpu.roll(sums[2], count - 1, 0))
    return (before + sums[1] + after).reshape(lines, depth, sums[0].shape[1])


def tap(step, odd):
    return step + odd * (2 - 2 * step)


def inner_rows(chans, size_y):
    return {1: (0, size_y), 2: (lax.axis_index("chan"), size_y - 1)}.get(chans, (1, size_y - 2))


def border_rows(chans, size_y):
    if chans == 1:
        return []
    if chans == 2:
        return [(jnp.where(lax.axis_index("chan") == 0, size_y - 1, -1), 2)]
    return [(-1, 2), (size_y - 1, 2)]


def fill_inner(target, planes, valid=None):
    size_y = target.shape[1] - 2
    zeros = jnp.zeros(target.shape[2:], target.dtype)
    for slot, (block, plane) in enumerate(planes):
        rows = block[...] if plane is None else block[plane]
        target[slot, 0] = zeros
        target[slot, 1 : size_y + 1] = rows if valid is None else jnp.where(valid, rows, jnp.zeros_like(rows))
        target[slot, size_y + 1] = zeros


def fill_border(target, start, size_y, planes, valid=None):
    high = start > 0
    place, source = jnp.where(high, 0, 2), jnp.where(high, size_y - 2, 0)
    for slot, (block, plane, halo, halo_plane) in enumerate(planes):
        rows = block[pl.ds(source, 2)] if plane is None else block[plane, pl.ds(source, 2)]
        beyond = halo[halo_plane]
        if valid is not None:
            rows = jnp.where(valid, rows, jnp.zeros_like(rows))
            beyond = jnp.where(valid, beyond, jnp.zeros_like(beyond))
        target[slot, pl.ds(place, 2)] = rows
        target[slot, pl.ds(2 - place, 2)] = beyond


def clear_outside(layer, slot, chans):
    chan = lax.axis_index("chan")
    last = layer.shape[1] - 1
    for row, owner in ((0, 0), (last, chans - 1)):
        if chans <= 2:
            keep = jnp.logical_and(chans == 2, chan != owner)
        else:
            keep = chan != owner
        layer[slot, row] = jnp.where(keep, layer[slot, row], jnp.zeros_like(layer[slot, row]))


def kernel_a0(own, near, weight_one, done_three, done_four, part_one, part_two, field, *, chans):
    odd = lax.rem(lax.axis_index("brick"), 2)
    size_y = own.shape[1]
    fill_inner(field, ((own, odd), (own, 1 - odd), (near, odd), (near, 1 - odd)))
    first, rows = inner_rows(chans, size_y)
    lines = tile_of(rows)
    for row in range(0, rows, lines):
        spot, base = pl.ds(row, lines), first + row
        for slot, done in enumerate((done_three, done_four)):
            terms = [(field, slot + step, tap(step, odd)) for step in range(3)]
            done[spot] = jnp.maximum(conv_lines(terms, base, lines, weight_one), 0.0).astype(BF16)
        terms = [(field, 0, tap(1, odd)), (field, 1, tap(2, odd))]
        part_two[spot] = conv_lines(terms, base, lines, weight_one)
        part_one[spot] = conv_lines([(field, 0, tap(2, odd))], base, lines, weight_one)


def kernel_a1(*refs, chans, sides):
    own, own_halos = refs[0], refs[1 : 1 + sides]
    near, near_halos = refs[1 + sides], refs[2 + sides : 2 + 2 * sides]
    done_three, done_four, weight_one, weight_two = refs[2 + 2 * sides : 6 + 2 * sides]
    out_two, out_three = refs[6 + 2 * sides : 8 + 2 * sides]
    parts = refs[8 + 2 * sides : 8 + 4 * sides]
    field, layer = refs[8 + 4 * sides :]
    odd = lax.rem(lax.axis_index("brick"), 2)
    size_y = own.shape[1]
    first, rows = inner_rows(chans, size_y)
    layer[0, pl.ds(first + 1, rows)] = done_three[...]
    layer[1, pl.ds(first + 1, rows)] = done_four[...]
    for side, (start, count) in enumerate(border_rows(chans, size_y)):
        pairs = ((own, own_halos[side], odd), (own, own_halos[side], 1 - odd))
        pairs += ((near, near_halos[side], odd), (near, near_halos[side], 1 - odd))
        fill_border(field, start, size_y, [(block, plane, halo, plane) for block, halo, plane in pairs])
        for slot in range(2):
            terms = [(field, slot + step, tap(step, odd)) for step in range(3)]
            value = jnp.maximum(conv_lines(terms, 0, count, weight_one), 0.0).astype(BF16)
            layer[slot, pl.ds(start + 1, count)] = value
        terms = [(field, 0, tap(1, odd)), (field, 1, tap(2, odd))]
        parts[sides + side][...] = conv_lines(terms, 0, count, weight_one)
        parts[side][...] = conv_lines([(field, 0, tap(2, odd))], 0, count, weight_one)
    for slot in range(2):
        clear_outside(layer, slot, chans)
    lines = tile_of(size_y)
    for row in range(0, size_y, lines):
        spot = pl.ds(row, lines)
        out_two[spot] = conv_lines([(layer, 0, tap(2, odd))], row, lines, weight_two)
        out_three[spot] = conv_lines([(layer, 0, tap(1, odd)), (layer, 1, tap(2, odd))], row, lines, weight_two)


def kernel_m(plane_one, part_one, part_two, weight_one, more_one, done_two, field, *, chans):
    odd = lax.rem(lax.axis_index("brick"), 2)
    fill_inner(field, ((plane_one, None),), has_far())
    first, rows = inner_rows(chans, plane_one.shape[0])
    lines = tile_of(rows)
    for row in range(0, rows, lines):
        spot, base = pl.ds(row, lines), first + row
        value = conv_lines([(field, 0, tap(0, odd))], base, lines, weight_one)
        done_two[spot] = jnp.maximum(value + part_two[spot], 0.0).astype(BF16)
        more_one[spot] = part_one[spot] + conv_lines([(field, 0, tap(1, odd))], base, lines, weight_one)


def kernel_b0(plane_zero, part_one, weight_one, done_one, field, *, chans):
    odd = lax.rem(lax.axis_index("brick"), 2)
    valid = has_far()
    fill_inner(field, ((plane_zero, None),), valid)
    first, rows = inner_rows(chans, plane_zero.shape[0])
    lines = tile_of(rows)
    for row in range(0, rows, lines):
        spot = pl.ds(row, lines)
        value = conv_lines([(field, 0, tap(0, odd))], first + row, lines, weight_one)
        done_one[spot] = jnp.where(valid, jnp.maximum(value + part_one[spot], 0.0), 0.0).astype(BF16)


def kernel_b1(*refs, chans, sides):
    plane_one, plane_zero, halos = refs[0], refs[1], refs[2 : 2 + sides]
    done_one, done_two, out_two, out_three, weight_one, weight_two = refs[2 + sides : 8 + sides]
    parts = refs[8 + sides : 8 + 3 * sides]
    skipped_two, skipped_three, pooled, field, layer, sums = refs[8 + 3 * sides :]
    odd = lax.rem(lax.axis_index("brick"), 2)
    valid = has_far()
    size_y, depth = plane_one.shape[0], plane_one.shape[1]
    first, rows = inner_rows(chans, size_y)
    layer[0, pl.ds(first + 1, rows)] = done_one[...]
    layer[1, pl.ds(first + 1, rows)] = done_two[...]
    for side, (start, count) in enumerate(border_rows(chans, size_y)):
        planes = ((plane_zero, None, halos[side], odd), (plane_one, None, halos[side], 1 - odd))
        fill_border(field, start, size_y, planes, valid)
        value = conv_lines([(field, 0, tap(0, odd)), (field, 1, tap(1, odd))], 0, count, weight_one)
        value = jnp.maximum(value + parts[side][...], 0.0)
        layer[0, pl.ds(start + 1, count)] = jnp.where(valid, value, 0.0).astype(BF16)
        value = conv_lines([(field, 1, tap(0, odd))], 0, count, weight_one)
        layer[1, pl.ds(start + 1, count)] = jnp.maximum(value + parts[sides + side][...], 0.0).astype(BF16)
    for slot in range(2):
        clear_outside(layer, slot, chans)
    lines = tile_of(size_y)
    for row in range(0, size_y, lines):
        spot = pl.ds(row, lines)
        value = conv_lines([(layer, 0, tap(0, odd)), (layer, 1, tap(1, odd))], row, lines, weight_two)
        two = jnp.maximum(value + out_two[spot], 0.0).astype(BF16)
        skipped_two[spot] = two
        value = conv_lines([(layer, 1, tap(0, odd))], row, lines, weight_two)
        three = jnp.maximum(value + out_three[spot], 0.0).astype(BF16)
        skipped_three[spot] = three
        both = two.astype(F32) + three.astype(F32)
        for group in range(sums.shape[0]):
            sums[group, spot] = both[:, :, group * LANES : (group + 1) * LANES]
    for row in range(size_y // 2):
        for group in range(sums.shape[0]):
            pairs = [
                sums[group, 2 * row + step, pl.ds(side, depth // 2, stride=2)] for step in range(2) for side in range(2)
            ]
            mean = (pairs[0] + pairs[1] + pairs[2] + pairs[3]) * 0.125
            pooled[row, :, group * LANES : (group + 1) * LANES] = mean.astype(BF16)


def fill_pooled(target, planes, valid=None):
    chan, chans = lax.axis_index("chan"), len(planes[0])
    zeros = jnp.zeros(target.shape[2:], target.dtype)
    for slot, blocks in enumerate(planes):
        rows = blocks[0].shape[0]
        target[slot, 0] = zeros
        target[slot, chans * rows + 1] = zeros
        for step, block in enumerate(blocks):
            source = lax.rem(chan - step + chans, chans)
            value = block[...]
            if valid is not None:
                value = jnp.where(valid, value, jnp.zeros_like(value))
            target[slot, pl.ds(1 + source * rows, rows)] = value


def kernel_c1(*refs, chans):
    weight, part, field = refs[2 * chans :]
    odd = lax.rem(lax.axis_index("brick"), 2)
    fill_pooled(field, (refs[:chans], refs[chans : 2 * chans]))
    lines = tile_of(part.shape[0])
    for row in range(0, part.shape[0], lines):
        part[pl.ds(row, lines)] = conv_lines([(field, 0, tap(1, odd)), (field, 1, tap(2, odd))], row, lines, weight)


def kernel_c2(*refs, chans, steps):
    part, weight, projection = refs[chans : chans + 3]
    results, field = refs[chans + 3 : -1], refs[-1]
    odd = lax.rem(lax.axis_index("brick"), 2)
    total, depth = part.shape[0], part.shape[1]
    rows = total // chans
    fill_pooled(field, (refs[:chans],), has_far())
    lines = tile_of(rows)
    for step, result in zip(steps, results):
        start = lax.rem(lax.axis_index("chan") + step, chans) * rows
        for row in range(0, rows, lines):
            value = conv_lines([(field, 0, tap(0, odd))], start + row, lines, weight)
            value = jnp.maximum(value + part[pl.ds(start + row, lines)], 0.0).astype(BF16)
            value = value.reshape(lines * depth, weight.shape[4])
            lifted = jnp.dot(value, projection[...], preferred_element_type=F32)
            result[pl.ds(row, lines)] = lifted.reshape(lines, depth, lifted.shape[1]).astype(result.dtype)


def kernel_d(*refs):
    skipped_two, skipped_three, own_part = refs[:3]
    received, merged, fine = refs[3:-2], refs[-2], refs[-1]
    odd = lax.rem(lax.axis_index("brick"), 2)
    rows, depth = own_part.shape[0], own_part.shape[1]
    lifted = own_part[...]
    for part in received:
        lifted = lifted + part[...].astype(F32)
    for group in range(fine.shape[0]):
        lanes = slice(group * LANES, (group + 1) * LANES)
        for row in range(rows):
            for side in range(2):
                fine[group, row, pl.ds(side, depth, stride=2)] = lifted[row, :, lanes]
        for row in range(rows):
            value = fine[group, row]
            for plane, skipped in ((odd, skipped_two), (1 - odd, skipped_three)):
                for step in range(2):
                    line = 2 * row + step
                    merged[plane, line, :, lanes] = (skipped[line, :, lanes].astype(F32) + value).astype(BF16)


def shards(volume, first_weight, second_weight, coarse_weight, projection):
    chans = lax.axis_size("chan")
    size_x, size_y, depth, channels = volume.shape
    assert size_x == 2 and lax.axis_size("brick") % 2 == 0

    turns = [[], [lambda c: 1 - c]][chans - 1] if chans <= 2 else [lambda c: c + 1, lambda c: c - 1]
    near = exchange(volume, "near")
    token = call(early, [], [((8, LANES), F32)], [], WEIGHT_COPY_FLOPS, 4)[0]
    plane_shape, sides = (size_y, depth, channels), len(turns)
    first, second, *edges = call(
        functools.partial(pieces_to_send, chans=chans),
        [volume, token],
        [(plane_shape, BF16)] * 2 + [((2, 2, depth, channels), BF16)] * sides,
        [],
        WEIGHT_COPY_FLOPS,
        4,
    )
    own_halos = [exchange(edge, "own", turn) for edge, turn in zip(edges, turns)]
    far_one = exchange(first, "far")
    far_halos = [exchange(halo, "far") for halo in own_halos]
    far_zero = exchange(second, "far")
    near_halos = [exchange(halo, "near") for halo in own_halos]

    static = dict(chans=chans, sides=sides)
    inner = inner_rows(chans, size_y)[1]
    border_shape = (2, depth, channels)
    line_flops = 2 * depth * 9 * channels * channels
    done_three, done_four, part_one, part_two = call(
        functools.partial(kernel_a0, chans=chans),
        [volume, near, first_weight],
        [((inner, depth, channels), BF16)] * 2 + [((inner, depth, channels), F32)] * 2,
        [pltpu.VMEM((4, size_y + 2, depth, channels), BF16)],
        9 * inner * line_flops,
        12,
    )
    part_one, done_two = call(
        functools.partial(kernel_m, chans=chans),
        [far_one, part_one, part_two, first_weight],
        [((inner, depth, channels), F32), ((inner, depth, channels), BF16)],
        [pltpu.VMEM((1, size_y + 2, depth, channels), BF16)],
        2 * inner * line_flops,
        12,
    )
    out_two, out_three, *border = call(
        functools.partial(kernel_a1, **static),
        [volume, *own_halos, near, *near_halos, done_three, done_four, first_weight, second_weight],
        [(plane_shape, F32)] * 2 + [(border_shape, F32)] * (2 * sides),
        [pltpu.VMEM((4, 4, depth, channels), BF16), pltpu.VMEM((2, size_y + 2, depth, channels), BF16)],
        (18 * sides + 3 * size_y) * line_flops,
        12,
    )
    done_one = call(
        functools.partial(kernel_b0, chans=chans),
        [far_zero, part_one, first_weight],
        [((inner, depth, channels), BF16)],
        [pltpu.VMEM((1, size_y + 2, depth, channels), BF16)],
        inner * line_flops,
        12,
    )[0]
    skipped_two, skipped_three, pooled = call(
        functools.partial(kernel_b1, **static),
        [far_one, far_zero, *far_halos, done_one, done_two, out_two, out_three, first_weight, second_weight, *border],
        [(plane_shape, BF16)] * 2 + [((size_y // 2, depth // 2, channels), BF16)],
        [
            pltpu.VMEM((2, 4, depth, channels), BF16),
            pltpu.VMEM((2, size_y + 2, depth, channels), BF16),
            pltpu.VMEM((channels // LANES, size_y, depth, LANES), F32),
        ],
        (6 * sides + 3 * size_y) * line_flops,
        12,
    )

    turns = [(lambda c, step=step: (c + step) % chans) for step in range(chans)]
    own_blocks = [pooled] + [exchange(pooled, "own", turn) for turn in turns[1:]]
    far_blocks = [exchange(pooled, "far", turn) for turn in turns[1:]]
    far_blocks = [exchange(pooled, "far")] + far_blocks
    near_blocks = [exchange(pooled, "near")]
    near_blocks += [exchange(block, "near") for block in own_blocks[1:]]
    part_shape = (size_y // 2, depth // 2, channels)
    coarse_rows = chans * size_y // 2
    coarse_channels = coarse_weight.shape[4]
    plane_flops = 2 * coarse_rows * (depth // 2) * 9 * channels * coarse_channels
    coarse_field = (coarse_rows + 2, depth // 2, channels)
    coarse_part = call(
        functools.partial(kernel_c1, chans=chans),
        [*own_blocks, *near_blocks, coarse_weight],
        [((coarse_rows, depth // 2, coarse_channels), F32)],
        [pltpu.VMEM((2,) + coarse_field, BF16)],
        2 * plane_flops,
        12,
    )[0]
    def last_part(steps, dtype):
        return call(
            functools.partial(kernel_c2, chans=chans, steps=steps),
            [*far_blocks, coarse_part, coarse_weight, projection],
            [(part_shape, dtype)] * len(steps),
            [pltpu.VMEM((1,) + coarse_field, BF16)],
            plane_flops * len(steps) // chans,
            12,
        )

    received = []
    if chans > 1:
        sent = last_part(tuple(range(1, chans)), BF16)
        received = [exchange(part, "own", turn) for part, turn in zip(sent, turns[1:])]
    own_part = last_part((0,), F32)[0]
    return call(
        kernel_d,
        [skipped_two, skipped_three, own_part, *received],
        [(volume.shape, BF16)],
        [pltpu.VMEM((channels // LANES, size_y // 2, depth, LANES), F32)],
        volume.size,
        16,
        results_in_vmem=False,
    )[0]


def solution(mesh):
    in_specs = (
        P("brick", "chan", None, None),
        P(),
        P(),
        P(None, None, None, None, "chan"),
        P("chan", None),
    )
    out_specs = P("brick", "chan", None, None)

    return jax.shard_map(shards, mesh=mesh, in_specs=in_specs, out_specs=out_specs, check_vma=False)
```
